1024 devices in a mesh: group: 2 (over core), rep: 32 (over x, z_lo), tp: 16 (over y, z_hi).
Axes of the slice: x: 4, y: 4, z: 32 (z_hi: 4, z_lo: 8; z = z_hi * 8 + z_lo), core: 2. Of those that a mesh axis runs over, the one named last changes fastest.
Arguments:
- master_weight: float32 [8192, 1024], P(('group', 'rep', 'tp')), may hold values from -0.25 to 0.25
- grad: float32 [8192, 1024], P(('group', 'rep', 'tp')), may hold values from -0.015625 to 0.015625
- moment1: float32 [8192, 1024], P(('group', 'rep', 'tp')), may hold values from -0.015625 to 0.015625
- moment2: float32 [8192, 1024], P(('group', 'rep', 'tp')), may hold values from 1e-08 to 1e-06
- step_count: int32 [1], replicated, may hold values from 1 to 299
- x_new: bfloat16 [4, 256, 8192], P(None, ('group', 'rep')), may hold values from -6 to 6
- queries: bfloat16 [4, 256, 8192], P(None, ('group', 'rep')), may hold values from -132 to 132
- new_keys: bfloat16 [4, 256, 1024], P(None, ('group', 'rep')), may hold values from -6 to 6
- cache_keys: bfloat16 [256, 1024, 1024], P(('group', 'rep'), 'tp'), may hold values from -6 to 6
- cache_values: bfloat16 [256, 1024, 1024], P(('group', 'rep'), 'tp'), may hold values from -6 to 6
- lengths: int32 [64, 4], P(('group', 'rep')), may hold values from 1 to 1024, 2560 in all within a row
Outputs:
- new_weight: float32 [8192, 1024], P(('group', 'rep', 'tp'))
- channel_scale: float32 [1024], P('tp')
- fresh_values: bfloat16 [4, 256, 1024], P(None, ('group', 'rep'), 'tp')
- attention: float32 [4, 256, 8192], P(None, ('group', 'rep'), 'tp')
The draws below stay inside these ranges and needn't reach their ends.
Inputs may be any that keep to these rules, and one draw needn't show every extreme that they name: `lengths`: within each replica's 4 sequences at least one has exactly 1024 live positions.
All inputs are finite; a program needn't handle non-finite values.
Results may differ from the reference program's by a relative error of at most 0.0055.
Values may be sent and summed in bfloat16 or wider, within the bound.
A program may use at most 64 MiB of HBM per device.

```python
import math
import jax
import jax.numpy as jnp
import numpy as np
from jax import lax

D = 8192
H = 64
KV = 8
HD = 128
BR = 4
L = 1024
STEPS = 4
KVW = 1024
NREP = 64
ROWS = 256


def keys_queries(key):
    base_key = jax.random.fold_in(key, 7)
    keys = jnp.clip(jax.random.normal(jax.random.fold_in(base_key, 1), (ROWS, L, KV * HD), jnp.float32), -6.0, 6.0)
    queries = jnp.clip(jax.random.normal(jax.random.fold_in(base_key, 2), (STEPS, ROWS, H * HD), jnp.float32), -6.0, 6.0)
    return (keys, queries)


def draw_cache_keys(key, part):
    return keys_queries(key)[0].astype(jnp.bfloat16)


def draw_queries(key, part):
    return keys_queries(key)[1].astype(jnp.bfloat16)


def strengthened(drawn, stream_key, source, target, shards_of, factor):
    owner, partner = [(jnp.arange(drawn.shape[axis_at]) // (drawn.shape[axis_at] // shards_of)).reshape([-1 if axis == axis_at else 1 for axis in range(drawn.ndim)]) for axis_at in (source, target)]
    chosen = jax.random.permutation(stream_key, shards_of)[partner]
    strong = (owner == chosen) | (owner == (partner + shards_of // 2) % shards_of)
    return jnp.where(strong, factor * drawn, drawn)


def block_scale(own_key, dims, shards, smallest, largest):
    level, own = 1.0, jax.random.fold_in(own_key, 6)
    for position, parts in shards:
        steps = jnp.exp(jax.random.uniform(jax.random.fold_in(own, position), (parts,), jnp.float32, smallest / len(shards), largest / len(shards)))
        level = level * jnp.repeat(steps, dims[position] // parts).reshape([-1 if axis == position else 1 for axis in range(len(dims))])
    return level


def length_profile(amount, total, reach, lean):
    weights = [(1 << 20) // math.isqrt(rank ** lean) + 1 for rank in range(2, amount + 1)]
    spare, given = total - reach - (amount - 1), [1] * (amount - 1)
    while spare > 0:
        movable = [i for i in range(amount - 1) if given[i] < reach]
        pool, budget = sum([weights[i] for i in movable]), spare
        for i in movable:
            extra = min(reach - given[i], max(1, budget * weights[i] // pool), spare)
            given[i] = given[i] + extra
            spare = spare - extra
    return np.array([reach] + given)


def ragged(stream_key, count, total, reach, lean):
    if count == 2:
        one = jax.random.randint(stream_key, (), max(1, total - reach), min(reach, total - 1) + 1)
        return jnp.stack([one, total - one])
    sizes = jnp.asarray(length_profile(count, total, reach, lean), jnp.int32)
    twos = (count - 1) // 2
    source_of, sink = sizes[1:1 + 2 * twos:2], sizes[2:2 + 2 * twos:2]
    margin = jnp.minimum(source_of - 1, reach - sink)
    shifted = jax.random.randint(jax.random.fold_in(stream_key, 1), (twos,), 0, 1 << 20) % (margin + 1)
    sizes = sizes.at[1:1 + 2 * twos:2].set(source_of - shifted).at[2:2 + 2 * twos:2].set(sink + shifted)
    return sizes[jax.random.permutation(jax.random.fold_in(stream_key, 2), count)]


def scatter_about(key, dims, spread, bound, cuts=(), kind=jnp.bfloat16):
    loudness = block_scale(key, dims, cuts, -0.22, 0.18) if cuts else 1.0
    values = jax.random.normal(key, dims, jnp.float32) * spread * loudness
    return jnp.minimum(jnp.maximum(values, -bound), bound).astype(kind)


def noise_with(stream_key, shape, scale, bound, cuts, heavy, kind=jnp.bfloat16):
    values = scale * jax.random.normal(stream_key, shape, jnp.float32)
    if cuts:
        values = values * block_scale(stream_key, shape, cuts, -0.22, 0.18)
    return jnp.clip(strengthened(values, jax.random.fold_in(stream_key, 3), *heavy), -bound, bound).astype(kind)


def setup_inputs(seed: int = 0) -> dict:
    key_of = jax.random.split(jax.random.key(seed), 12)
    master_weight = noise_with(key_of[0], (D, KVW), D ** -0.5, 0.25, ((0, 1024),), (0, 1, 1024, 6.0), jnp.float32)
    grad = scatter_about(key_of[1], (D, KVW), 0.001, 0.015625, ((0, 1024),), jnp.float32)
    moment1 = scatter_about(key_of[2], (D, KVW), 0.001, 0.015625, ((0, 1024),), jnp.float32)
    moment2 = jnp.clip(jnp.exp(math.log(9.999999974752427e-07) - 4.6051702 * jax.random.uniform(key_of[3], (D, KVW), jnp.float32) ** block_scale(key_of[3], (D, KVW), ((0, 1024),), -0.2, 0.2)), 9.99999993922529e-09, 9.999999974752427e-07)
    step_count = jax.random.randint(key_of[4], (1,), 1, 300).astype(jnp.int32)
    x_new = scatter_about(key_of[5], (STEPS, ROWS, D), 1.0, 6.0, ((1, 64),))
    queries = draw_queries(jax.random.fold_in(key_of[11], 71), 0)
    new_keys = scatter_about(key_of[7], (STEPS, ROWS, KVW), 1.0, 6.0, ((1, 64),))
    cache_keys = draw_cache_keys(jax.random.fold_in(key_of[11], 71), 0)
    cache_values = scatter_about(key_of[9], (ROWS, L, KVW), 1.0, 6.0, ((0, 64), (1, 16)))
    lengths = jax.vmap(lambda own: ragged(own, BR, BR * L * 5 // 8, L, 2))(jax.random.split(key_of[10], NREP)).reshape((NREP, BR)).astype(jnp.int32)
    return dict(master_weight=master_weight, grad=grad, moment1=moment1, moment2=moment2, step_count=step_count, x_new=x_new, queries=queries, new_keys=new_keys, cache_keys=cache_keys, cache_values=cache_values, lengths=lengths)


beta_first = 0.9
beta_second = 0.999
learn_rate = 0.01
decay_rate = 0.1
adam_floor = 1e-08
scale_floor = 1e-06
code_range = 448.0
masked_score = -1e+30

def adamw(master_weight, grad, moment1, moment2, step_count):
    steps_done = step_count[0].astype(jnp.float32)
    first = beta_first * moment1 + (1.0 - beta_first) * grad
    second = beta_second * moment2 + (1.0 - beta_second) * grad * grad
    correction = jnp.sqrt(1.0 - jnp.exp(steps_done * math.log(beta_second))) / (1.0 - jnp.exp(steps_done * math.log(beta_first)))
    return master_weight - learn_rate * correction * first / (jnp.sqrt(second) + adam_floor) - learn_rate * decay_rate * master_weight

def attend_replica(inputs):
    queries, new_keys, fresh_values, cache_keys, cache_values, lengths = inputs
    group_size = H // KV
    hp = lax.Precision.HIGHEST
    query_grid = queries.astype(jnp.float32).reshape(STEPS, BR, KV, group_size, HD).transpose(1, 2, 3, 0, 4)
    key_grid = cache_keys.astype(jnp.float32).reshape(BR, L, KV, HD)
    value_grid = cache_values.astype(jnp.float32).reshape(BR, L, KV, HD)
    fresh_key_grid = new_keys.astype(jnp.float32).reshape(STEPS, BR, KV, HD).transpose(1, 2, 0, 3)
    fresh_value_grid = fresh_values.astype(jnp.float32).reshape(STEPS, BR, KV, HD).transpose(1, 2, 0, 3)
    inverse = 1.0 / math.sqrt(HD)
    cache_scores = jnp.einsum('bkgsd,bpkd->bkgsp', query_grid, key_grid, precision=hp) * inverse
    fresh_scores = jnp.einsum('bkgsd,bkjd->bkgsj', query_grid, fresh_key_grid, precision=hp) * inverse
    live = (jnp.arange(L, dtype=jnp.int32)[None, :] < lengths[:, None])[:, None, None, None, :]
    causal = jnp.arange(STEPS, dtype=jnp.int32)[:, None] >= jnp.arange(STEPS, dtype=jnp.int32)[None, :]
    peak_score = jnp.maximum(lax.optimization_barrier(jnp.max(jnp.where(live, cache_scores, masked_score), axis=-1)), lax.optimization_barrier(jnp.max(jnp.where(causal, fresh_scores, masked_score), axis=-1)))
    cache_weights = jnp.where(live, jnp.exp(cache_scores - peak_score[..., None]), 0.0)
    fresh_weights = jnp.where(causal, jnp.exp(fresh_scores - peak_score[..., None]), 0.0)
    denominator = lax.optimization_barrier(jnp.sum(cache_weights, axis=-1)) + lax.optimization_barrier(jnp.sum(fresh_weights, axis=-1))
    cache_rounded = lax.optimization_barrier(cache_weights.astype(jnp.bfloat16)).astype(jnp.float32)
    fresh_rounded = lax.optimization_barrier(fresh_weights.astype(jnp.bfloat16)).astype(jnp.float32)
    mixed = jnp.einsum('bkgsp,bpkd->bkgsd', cache_rounded, value_grid, precision=hp)
    mixed = mixed + jnp.einsum('bkgsj,bkjd->bkgsd', fresh_rounded, fresh_value_grid, precision=hp)
    result = mixed / denominator[..., None]
    return result.transpose(3, 0, 1, 2, 4).reshape(STEPS, BR, H * HD)

def reference(master_weight, grad, moment1, moment2, step_count, x_new, queries, new_keys, cache_keys, cache_values, lengths):
    new_weight = adamw(master_weight, grad, moment1, moment2, step_count)
    channel_scale = (lax.optimization_barrier(jnp.max(jnp.abs(new_weight), axis=0)) + scale_floor) / code_range
    coded = (new_weight / channel_scale).astype(jnp.bfloat16)
    total_rows = x_new.shape[1]
    replicas = total_rows // BR
    flat = x_new.reshape(STEPS * total_rows, D)
    fresh_values = (jnp.dot(flat, coded, preferred_element_type=jnp.float32) * channel_scale).astype(jnp.bfloat16)
    fresh_values = fresh_values.reshape(STEPS, total_rows, KV * HD)

    def by_replica(array, width):
        return array.reshape(STEPS, replicas, BR, width).transpose(1, 0, 2, 3)
    inputs = (by_replica(queries, H * HD), by_replica(new_keys, KV * HD), by_replica(fresh_values, KV * HD), cache_keys.reshape(replicas, BR, L, KV * HD), cache_values.reshape(replicas, BR, L, KV * HD), lengths)
    outputs = lax.map(attend_replica, inputs)
    attention = outputs.transpose(1, 0, 2, 3).reshape(STEPS, total_rows, H * HD)
    return (new_weight, channel_scale, fresh_values, attention)
```

```python
import functools
import math

import jax
import jax.numpy as jnp
from jax import lax
from jax.experimental import pallas as pl
from jax.experimental.pallas import tpu as pltpu
from jax.sharding import PartitionSpec as P

H = 64
KV = 8
HD = 128
STEPS = 4
BR = 4

beta_first = 0.9
beta_second = 0.999
learn_rate = 0.01
decay_rate = 0.1
adam_floor = 1e-08
scale_floor = 1e-06
code_range = 448.0
masked_score = -1e30

F32 = jnp.float32
BF16 = jnp.bfloat16
MESH = pl.DeviceIdType.MESH

NX, NY, ZLO, ZHI = 4, 4, 8, 4
NZ = ZLO * ZHI
WINDOW = (1, -1, 2, -2, 3, -3, 4)


def kernel(
    mw_ref,
    grad_ref,
    m1_ref,
    m2_ref,
    step_ref,
    x_ref,
    q_ref,
    nk_ref,
    k_ref,
    v_ref,
    len_ref,
    nw_ref,
    scale_ref,
    fresh_ref,
    att_ref,
    w_buf,
    xp_buf,
    sel_mat,
    mask_buf,
    ya_buf,
    ys_buf,
    yar_buf,
    ysr_buf,
    za_buf,
    zs_buf,
    zar_buf,
    zsr_buf,
    cs_buf,
    cr_buf,
    yf_buf,
    yfr_buf,
    zf_buf,
    zfr_buf,
    win_send,
    win_recv,
    x_send,
    x_recv,
    xp_sem,
    c_sem,
    y_send,
    y_recv,
    z_send,
    z_recv,
):
    g = lax.axis_index("group")
    rep = lax.axis_index("rep")
    tp = lax.axis_index("tp")
    x, zl = rep // ZLO, rep % ZLO
    y, zh = tp // ZHI, tp % ZHI
    z = zh * ZLO + zl

    def at_z(offset):
        there = (z + offset + NZ) % NZ
        return {"rep": x * ZLO + there % ZLO, "tp": y * ZHI + there // ZLO}

    def at_x(offset):
        return {"rep": ((x + offset + NX) % NX) * ZLO + zl}

    def at_y(offset):
        return {"tp": ((y + offset) % NY) * ZHI + zh}

    partner = {"group": 1 - g}

    barrier = pltpu.get_barrier_semaphore()
    peers = [at_z(d) for d in (8, 24, 16, 4, -4, 3, -3, 2, -2, 1, -1)]
    peers += [at_y(d) for d in (2, 1, 3)] + [at_x(d) for d in (1, -1)] + [partner]
    for peer in peers:
        pl.semaphore_signal(barrier, inc=1, device_id=peer, device_id_type=MESH)

    def remote(src, dst, send, recv, peer):
        return pltpu.make_async_remote_copy(
            src_ref=src, dst_ref=dst, send_sem=send, recv_sem=recv, device_id=peer, device_id_type=MESH
        )

    steps_done = jnp.full((8, 1024), step_ref[0], jnp.int32).astype(F32)
    first = beta_first * m1_ref[...] + (1.0 - beta_first) * grad_ref[...]
    second = beta_second * m2_ref[...] + (1.0 - beta_second) * grad_ref[...] * grad_ref[...]
    correction = jnp.sqrt(1.0 - jnp.exp(steps_done * math.log(beta_second))) / (
        1.0 - jnp.exp(steps_done * math.log(beta_first))
    )
    nw = (
        mw_ref[...]
        - learn_rate * correction * first / (jnp.sqrt(second) + adam_floor)
        - learn_rate * decay_rate * mw_ref[...]
    )
    nw_ref[...] = nw
    w_buf[x, zl] = jnp.concatenate([nw[:, :512], nw[:, 512:]], axis=0).astype(BF16)

    rows_b = []
    lane_b = lax.broadcasted_iota(jnp.int32, (64, 128), 1) % BR
    position = tp * 64 + lax.broadcasted_iota(jnp.int32, (64, 128), 0)
    for b in range(BR):
        live = jnp.logical_and(position < len_ref[0, b], lane_b == b)
        rows_b.append(jnp.where(live, 1.0, 0.0))
    mask_buf[...] = jnp.concatenate(rows_b, axis=0)
    inverse = 1.0 / math.sqrt(HD)

    def attend(kv, carry):
        base = kv * 1024
        queries = jnp.concatenate(
            [q_ref[:, pl.ds(pl.multiple_of(base + h * 128, 128), 128)] for h in range(8)], axis=0
        )
        columns = pl.ds(pl.multiple_of(kv * 128, 128), 128)
        scores = (
            lax.dot_general(
                k_ref[:, columns], queries, (((1,), (1,)), ((), ())), preferred_element_type=F32
            )
            * inverse
        )
        live = mask_buf[...] > 0.5
        masked = jnp.where(live, scores, masked_score)
        peak = jnp.max(masked, axis=0, keepdims=True)
        weights = jnp.where(live, jnp.exp(masked - peak), 0.0)
        total = jnp.sum(weights, axis=0, keepdims=True)
        part = lax.dot_general(
            v_ref[:, columns],
            weights.astype(BF16),
            (((0,), (0,)), ((), ())),
            preferred_element_type=F32,
        )
        ya_buf[kv] = part.astype(BF16)
        row = lax.broadcasted_iota(jnp.int32, (8, 128), 0)
        ys_buf[kv] = jnp.where(row == 0, peak, total)
        return carry

    lax.fori_loop(0, KV, attend, 0)

    for low in range(ZLO):
        there = (z + 28 + (low - z + 4 + NZ) % ZLO) % NZ
        lanes = (y * ZHI + there // ZLO) * 8
        r = lax.broadcasted_iota(jnp.int32, (128, 256), 0)
        c = lax.broadcasted_iota(jnp.int32, (128, 256), 1)
        k = c & 127
        hit = jnp.logical_and(
            jnp.logical_and((k >> 4) == low, ((k >> 3) & 1) == (c >> 7)), r == lanes + (k & 7)
        )
        sel_mat[low * 128 : (low + 1) * 128, :] = jnp.where(hit, 1.0, 0.0).astype(BF16)

    pl.semaphore_wait(barrier, len(peers))

    windows = []
    for i, d in enumerate(WINDOW):
        copy = remote(w_buf.at[x, zl], w_buf.at[x, zl], win_send.at[i], win_recv.at[i], at_z(d))
        copy.start()
        windows.append(copy)
    xp = remote(
        x_ref.at[:, pl.ds(pl.multiple_of((1 - g) * 4096, 4096), 4096)],
        xp_buf,
        xp_sem.at[0],
        xp_sem.at[1],
        partner,
    )
    xp.start()
    y_att = []
    for i, d in enumerate((1, 3, 2)):
        pair = pl.ds(((y + d) % NY) * 2, 2)
        y_att.append(
            (
                remote(ys_buf.at[pair], ysr_buf.at[i], y_send.at[0, i], y_recv.at[0, i], at_y(d)),
                remote(ya_buf.at[pair], yar_buf.at[i], y_send.at[1, i], y_recv.at[1, i], at_y(d)),
            )
        )
        for copy in y_att[-1]:
            copy.start()

    xp.wait_recv()
    pieces = []
    for other in range(NX):
        columns = pl.ds(pl.multiple_of((g * NX + other) * 1024, 1024), 1024)
        pieces += [x_ref[:, columns], xp_buf[:, other * 1024 : (other + 1) * 1024]]
    picked = jnp.dot(
        jnp.concatenate(pieces, axis=0), sel_mat[...], preferred_element_type=F32
    ).astype(BF16)
    sel_mat[0:128, :] = picked

    for copy in windows:
        copy.wait_recv()

    left, right = (x + NX - 1) % NX, (x + 1) % NX
    across = (x + 2) % NX
    to_right = remote(w_buf.at[x], w_buf.at[x], x_send.at[0], x_recv.at[0], at_x(1))
    to_left = remote(w_buf.at[x], w_buf.at[x], x_send.at[1], x_recv.at[1], at_x(-1))
    to_right.start()
    to_left.start()

    for copies in y_att:
        for copy in copies:
            copy.wait_recv()
    for pair in range(2):
        stats = [ys_buf[y * 2 + pair]] + [ysr_buf[i, pair] for i in range(3)]
        parts = [ya_buf[y * 2 + pair]] + [yar_buf[i, pair] for i in range(3)]
        peak = functools.reduce(jnp.maximum, [s[0:1] for s in stats])
        factors = [jnp.exp(s[0:1] - peak) for s in stats]
        total = sum(s[1:2] * f for s, f in zip(stats, factors))
        part = sum(p.astype(F32) * f for p, f in zip(parts, factors))
        row = lax.broadcasted_iota(jnp.int32, (8, 128), 0)
        zs_buf[pair] = jnp.where(row == 0, peak, total)
        turned = part.T.astype(BF16)
        za_buf[2 * pair] = turned[:64]
        za_buf[2 * pair + 1] = turned[64:]
    z_att = []
    for i, d in enumerate((2, 1, 3)):
        dest = (zh + d) % ZHI
        z_att.append(
            (
                remote(zs_buf.at[dest // 2], zsr_buf.at[i], z_send.at[0, i], z_recv.at[0, i], at_z(8 * d)),
                remote(za_buf.at[dest], zar_buf.at[i], z_send.at[1, i], z_recv.at[1, i], at_z(8 * d)),
            )
        )
        for copy in z_att[-1]:
            copy.start()

    def slab_product(other):
        lhs = sel_mat[pl.ds(pl.multiple_of(other * 32, 32), 32), :]
        lhs = jnp.concatenate([lhs[:, :128], lhs[:, 128:]], axis=0)
        slab = w_buf[other]
        top = jnp.max(jnp.abs(slab.astype(F32)), axis=0)
        return jnp.dot(lhs, slab.reshape(128, 512), preferred_element_type=F32), top

    partial, top = slab_product(x)
    to_right.wait_recv()
    on_right = remote(
        w_buf.at[left, pl.ds(0, 4)], w_buf.at[left, pl.ds(0, 4)], x_send.at[2], x_recv.at[2], at_x(1)
    )
    on_right.start()
    to_left.wait_recv()
    on_left = remote(
        w_buf.at[right, pl.ds(4, 4)], w_buf.at[right, pl.ds(4, 4)], x_send.at[3], x_recv.at[3], at_x(-1)
    )
    on_left.start()
    for other in (left, right):
        more, more_top = slab_product(other)
        partial, top = partial + more, jnp.maximum(top, more_top)
    on_right.wait_recv()
    on_left.wait_recv()
    more, more_top = slab_product(across)
    partial, top = partial + more, jnp.maximum(top, more_top)

    tops = [
        jnp.broadcast_to(jnp.max(top[h * 8 : h * 8 + 8], axis=0, keepdims=True), (8, 512))
        for h in range(2)
    ]
    for h in range(2):
        cs_buf[h, 0:16] = partial[h * 32 + 16 : h * 32 + 32]
        cs_buf[h, 16:24] = tops[h]
    core = remote(cs_buf, cr_buf, c_sem.at[0], c_sem.at[1], partner)
    core.start()
    core.wait_recv()
    for h in range(2):
        both = partial[h * 32 : h * 32 + 16] + cr_buf[h, 0:16]
        highest = jnp.maximum(tops[h], cr_buf[h, 16:24])
        for k in range(2):
            yf_buf[2 * h + k, 0:16] = both[:, k * 256 : (k + 1) * 256]
            yf_buf[2 * h + k, 16:24] = highest[:, k * 256 : (k + 1) * 256]
    y_new = []
    for i, d in enumerate((1, 3, 2)):
        copy = remote(yf_buf.at[(y + d) % NY], yfr_buf.at[i], y_send.at[2, i], y_recv.at[2, i], at_y(d))
        copy.start()
        y_new.append(copy)
    for copy in y_new:
        copy.wait_recv()
    blocks = [yf_buf[y]] + [yfr_buf[i] for i in range(3)]
    added = sum(b[0:16] for b in blocks)
    highest = functools.reduce(jnp.maximum, [b[16:24] for b in blocks])
    for k in range(2):
        zf_buf[k, 0:16] = added[:, k * 128 : (k + 1) * 128]
        zf_buf[k, 16:24] = highest[:, k * 128 : (k + 1) * 128]
    z_new = []
    for i, d in enumerate((2, 1, 3)):
        dest = (zh + d) % ZHI
        copy = remote(zf_buf.at[dest // 2], zfr_buf.at[i], z_send.at[2, i], z_recv.at[2, i], at_z(8 * d))
        copy.start()
        z_new.append(copy)

    head = y * 2 + zh // 2
    own_queries = jnp.concatenate(
        [q_ref[:, pl.ds(pl.multiple_of(head * 1024 + h * 128, 128), 128)] for h in range(8)], axis=0
    )
    own_keys = nk_ref[:, pl.ds(pl.multiple_of(head * 128, 128), 128)]
    new_scores = (
        lax.dot_general(own_keys, own_queries, (((1,), (1,)), ((), ())), preferred_element_type=F32)
        * inverse
    )
    r = lax.broadcasted_iota(jnp.int32, (16, 128), 0)
    c = lax.broadcasted_iota(jnp.int32, (16, 128), 1)
    causal = jnp.logical_and((r & 3) == (c & 3), (r >> 2) <= ((c >> 2) & 3))
    new_scores = jnp.where(causal, new_scores, masked_score)
    new_peak = jnp.max(new_scores, axis=0, keepdims=True)

    for copies in z_att:
        for copy in copies:
            copy.wait_recv()
    stats = [zs_buf[zh // 2]] + [zsr_buf[i] for i in range(3)]
    parts = [za_buf[zh]] + [zar_buf[i] for i in range(3)]
    peak = functools.reduce(jnp.maximum, [s[0:1] for s in stats] + [new_peak])
    factors = [jnp.exp(s[0:1] - peak) for s in stats]
    new_weights = jnp.where(causal, jnp.exp(new_scores - peak), 0.0)
    denominator = sum(s[1:2] * f for s, f in zip(stats, factors)) + jnp.sum(
        new_weights, axis=0, keepdims=True
    )
    share = 1.0 / denominator
    columns = jnp.concatenate([f * share for f in factors] + [share] * 4, axis=0).T
    odd = (zh % 2) == 1
    columns = jnp.where(odd, columns[64:], columns[:64])
    merged = sum(p.astype(F32) * columns[:, i : i + 1] for i, p in enumerate(parts))

    for copy in z_new:
        copy.wait_recv()
    blocks = [zf_buf[zh // 2]] + [zfr_buf[i] for i in range(3)]
    values = sum(b[0:16] for b in blocks).astype(BF16)
    highest = functools.reduce(jnp.maximum, [b[16:24] for b in blocks])
    scales = (highest + scale_floor) / code_range
    scale_ref[...] = jnp.where(odd, scales[:, 64:], scales[:, :64])
    wide = values.astype(F32)
    fresh_ref[...] = jnp.where(odd, wide[:, 64:], wide[:, :64]).astype(BF16)
    mixed = lax.dot_general(
        new_weights.astype(BF16), values, (((0,), (0,)), ((), ())), preferred_element_type=F32
    )
    mixed = jnp.where(odd, mixed[64:], mixed[:64])
    result = merged + mixed * columns[:, 4:5]
    for h in range(4):
        att_ref[:, h * 128 : (h + 1) * 128] = result[h * 16 : (h + 1) * 16]

    for copy in windows + [xp, to_right, to_left, on_right, on_left, core] + y_new + z_new:
        copy.wait_send()
    for copies in y_att + z_att:
        for copy in copies:
            copy.wait_send()


def body(
    master_weight,
    grad,
    moment1,
    moment2,
    step_count,
    x_new,
    queries,
    new_keys,
    cache_keys,
    cache_values,
    lengths,
):
    vmem = pl.BlockSpec(memory_space=pltpu.VMEM)
    smem = pl.BlockSpec(memory_space=pltpu.SMEM)
    dma = pltpu.SemaphoreType.DMA
    new_weight, scale, fresh, attention = pl.pallas_call(
        kernel,
        out_shape=(
            jax.ShapeDtypeStruct((8, 1024), F32),
            jax.ShapeDtypeStruct((8, 64), F32),
            jax.ShapeDtypeStruct((16, 64), BF16),
            jax.ShapeDtypeStruct((16, 512), F32),
        ),
        in_specs=[vmem] * 4 + [smem] + [vmem] * 5 + [smem],
        out_specs=(vmem,) * 4,
        scratch_shapes=[
            pltpu.VMEM((NX, ZLO, 16, 512), BF16),
            pltpu.VMEM((16, 4096), BF16),
            pltpu.VMEM((1024, 256), BF16),
            pltpu.VMEM((256, 128), F32),
            pltpu.VMEM((KV, 128, 128), BF16),
            pltpu.VMEM((KV, 8, 128), F32),
            pltpu.VMEM((3, 2, 128, 128), BF16),
            pltpu.VMEM((3, 2, 8, 128), F32),
            pltpu.VMEM((4, 64, 128), BF16),
            pltpu.VMEM((2, 8, 128), F32),
            pltpu.VMEM((3, 64, 128), BF16),
            pltpu.VMEM((3, 8, 128), F32),
            pltpu.VMEM((2, 24, 512), F32),
            pltpu.VMEM((2, 24, 512), F32),
            pltpu.VMEM((4, 24, 256), F32),
            pltpu.VMEM((3, 24, 256), F32),
            pltpu.VMEM((2, 24, 128), F32),
            pltpu.VMEM((3, 24, 128), F32),
            dma((7,)),
            dma((7,)),
            dma((4,)),
            dma((4,)),
            dma((2,)),
            dma((2,)),
            dma((3, 3)),
            dma((3, 3)),
            dma((3, 3)),
            dma((3, 3)),
        ],
        compiler_params=pltpu.CompilerParams(collective_id=0, has_side_effects=True),
    )(
        master_weight,
        grad,
        moment1,
        moment2,
        step_count,
        x_new.reshape(16, 8192),
        queries.reshape(16, 8192),
        new_keys.reshape(16, 1024),
        cache_keys.reshape(256, 1024),
        cache_values.reshape(256, 1024),
        lengths,
    )
    return (
        new_weight,
        scale[0],
        fresh.reshape(STEPS, BR, 64),
        attention.reshape(STEPS, BR, 512),
    )


def solution(mesh):
    return jax.shard_map(
        body,
        mesh=mesh,
        in_specs=(
            P(("group", "rep", "tp"), None),
            P(("group", "rep", "tp"), None),
            P(("group", "rep", "tp"), None),
            P(("group", "rep", "tp"), None),
            P(),
            P(None, ("group", "rep"), None),
            P(None, ("group", "rep"), None),
            P(None, ("group", "rep"), None),
            P(("group", "rep"), "tp", None),
            P(("group", "rep"), "tp", None),
            P(("group", "rep"), None),
        ),
        out_specs=(
            P(("group", "rep", "tp"), None),
            P("tp"),
            P(None, ("group", "rep"), "tp"),
            P(None, ("group", "rep"), "tp"),
        ),
        check_vma=False,
    )
```

```python
import functools
import math

import jax
import jax.numpy as jnp
from jax import lax
from jax.experimental import pallas as pl
from jax.experimental.pallas import tpu as pltpu
from jax.sharding import PartitionSpec as P

H = 64
KV = 8
HD = 128
STEPS = 4
BR = 4

beta_first = 0.9
beta_second = 0.999
learn_rate = 0.01
decay_rate = 0.1
adam_floor = 1e-08
scale_floor = 1e-06
code_range = 448.0
masked_score = -1e30

F32 = jnp.float32
BF16 = jnp.bfloat16
MESH = pl.DeviceIdType.MESH

NX, NY, ZLO, ZHI = 4, 4, 8, 4
NZ = ZLO * ZHI
SOURCES = (0, -1, 1, -2, 2, -3, 3, -4)


def adamw(mw, grad, m1, m2, step):
    steps_done = jnp.full(mw.shape, step, jnp.int32).astype(F32)
    first = beta_first * m1 + (1.0 - beta_first) * grad
    second = beta_second * m2 + (1.0 - beta_second) * grad * grad
    correction = jnp.sqrt(1.0 - jnp.exp(steps_done * math.log(beta_second))) / (
        1.0 - jnp.exp(steps_done * math.log(beta_first))
    )
    return mw - learn_rate * correction * first / (jnp.sqrt(second) + adam_floor) - learn_rate * decay_rate * mw


def kernel(
    mw_hbm,
    grad_hbm,
    m1_hbm,
    m2_hbm,
    step_ref,
    x_hbm,
    q_hbm,
    nk_hbm,
    k_hbm,
    v_hbm,
    len_ref,
    scale_ref,
    fresh_ref,
    att_ref,
    rows_buf,
    x4_buf,
    q4_buf,
    nk4_buf,
    k_ref,
    v_ref,
    xf_buf,
    q_ref,
    w_buf,
    xp_buf,
    sel_mat,
    pick_buf,
    mask_buf,
    ya_buf,
    ys_buf,
    yar_buf,
    ysr_buf,
    za_buf,
    zs_buf,
    zar_buf,
    zsr_buf,
    cs_buf,
    cr_buf,
    yf_buf,
    yfr_buf,
    zf_buf,
    zfr_buf,
    zm_buf,
    zmr_buf,
    in_sem,
    win_send,
    win_recv,
    x_send,
    x_recv,
    xp_sem,
    c_sem,
    y_send,
    y_recv,
    z_send,
    z_recv,
    hello,
):
    g = lax.axis_index("group")
    rep = lax.axis_index("rep")
    tp = lax.axis_index("tp")
    x, zl = rep // ZLO, rep % ZLO
    y, zh = tp // ZHI, tp % ZHI
    z = zh * ZLO + zl

    def at_z(offset):
        there = (z + offset + NZ) % NZ
        return {"rep": x * ZLO + there % ZLO, "tp": y * ZHI + there // ZLO}

    def at_x(offset):
        return {"rep": ((x + offset + NX) % NX) * ZLO + zl}

    def at_y(offset):
        return {"tp": ((y + offset) % NY) * ZHI + zh}

    partner = {"group": 1 - g}

    def signal(sem, peer):
        pl.semaphore_signal(sem, inc=1, device_id=peer, device_id_type=MESH)

    def remote(src, dst, send, recv, peer):
        return pltpu.make_async_remote_copy(
            src_ref=src, dst_ref=dst, send_sem=send, recv_sem=recv, device_id=peer, device_id_type=MESH
        )

    barrier = pltpu.get_barrier_semaphore()
    peers = [at_z(d) for d in (4, -4, 3, -3, 2, -2, 1, -1)]
    peers += [at_y(d) for d in (2, 1, 3)] + [at_x(d) for d in (1, -1)] + [partner]
    for peer in peers:
        signal(barrier, peer)

    loads = [
        pltpu.make_async_copy(src, dst, in_sem.at[i])
        for i, (src, dst) in enumerate(
            [(ref, rows_buf.at[i]) for i, ref in enumerate((mw_hbm, grad_hbm, m1_hbm, m2_hbm))]
            + [(q_hbm, q4_buf), (k_hbm, k_ref), (v_hbm, v_ref), (x_hbm, x4_buf), (nk_hbm, nk4_buf)]
        )
    ]
    for copy in loads:
        copy.start()

    for copy in loads[:4]:
        copy.wait()
    nw = adamw(rows_buf[0], rows_buf[1], rows_buf[2], rows_buf[3], step_ref[0])
    w_buf[x, zl] = jnp.concatenate([nw[:, :512], nw[:, 512:]], axis=0).astype(BF16)

    pl.semaphore_wait(barrier, len(peers))

    windows = [None]
    for i, e in enumerate(SOURCES):
        if e:
            own = w_buf.at[x, zl]
            copy = remote(own, own, win_send.at[i], win_recv.at[i], at_z(-e))
            copy.start()
            windows.append(copy)
    sent = []
    left, right, across = (x + NX - 1) % NX, (x + 1) % NX, (x + 2) % NX
    from_left, from_right, from_across = {}, {}, {}

    def block(owner, i):
        return w_buf.at[owner, (zl + SOURCES[i] + ZLO) % ZLO]

    def spread(i):
        ref = block(x, i)
        from_left[i] = remote(ref, ref, x_send.at[0, i], x_recv.at[0, i], at_x(1))
        from_right[i] = remote(ref, ref, x_send.at[1, i], x_recv.at[1, i], at_x(-1))
        from_left[i].start()
        from_right[i].start()

    def pass_on(i):
        from_left[i].wait_recv()
        from_right[i].wait_recv()
        if i % 2 == 0:
            ref = block(left, i)
            copy = remote(ref, ref, x_send.at[2, i], x_recv.at[2, i], at_x(1))
        else:
            ref = block(right, i)
            copy = remote(ref, ref, x_send.at[2, i], x_recv.at[2, i], at_x(-1))
        copy.start()
        from_across[i] = copy

    spread(0)
    half = pl.ds(pl.multiple_of((1 - g) * 4096, 4096), 4096)
    xp = remote(x_hbm.at[:, :, half], xp_buf, xp_sem.at[0], xp_sem.at[1], partner)
    xp.start()
    signal(hello.at[0], at_z(4))
    signal(hello.at[1], at_z(-4))

    rows_b = []
    lane_b = lax.broadcasted_iota(jnp.int32, (64, 128), 1) & 3
    position = tp * 64 + lax.broadcasted_iota(jnp.int32, (64, 128), 0)
    for b in range(BR):
        live = jnp.logical_and(position < len_ref[0, b], lane_b == b)
        rows_b.append(jnp.where(live, 1.0, 0.0))
    mask_buf[...] = jnp.concatenate(rows_b, axis=0)
    inverse = 1.0 / math.sqrt(HD)
    loads[4].wait()
    for s in range(STEPS):
        q_ref[4 * s : 4 * s + 4] = q4_buf[s].astype(F32)

    def head_queries(kv):
        return jnp.concatenate(
            [q_ref[:, pl.ds(pl.multiple_of(kv * 1024 + h * 128, 128), 128)] for h in range(8)], axis=0
        ).astype(BF16)

    def attend(kv, carry):
        columns = pl.ds(pl.multiple_of(kv * 128, 128), 128)
        scores = (
            lax.dot_general(
                k_ref[:, columns], head_queries(kv), (((1,), (1,)), ((), ())), preferred_element_type=F32
            )
            * inverse
        )
        live = mask_buf[...] > 0.5
        masked = jnp.where(live, scores, masked_score)
        peak = jnp.max(masked, axis=0, keepdims=True)
        weights = jnp.where(live, jnp.exp(masked - peak), 0.0)
        total = jnp.sum(weights, axis=0, keepdims=True)
        part = lax.dot_general(
            v_ref[:, columns],
            weights.astype(BF16),
            (((0,), (0,)), ((), ())),
            preferred_element_type=F32,
        )
        ya_buf[kv] = part.astype(BF16)
        ys_buf[kv] = jnp.concatenate([peak, total], axis=0)
        return carry

    loads[5].wait()
    loads[6].wait()
    lax.fori_loop(0, KV // 2, attend, 0)
    for i in (1, 2, 3):
        windows[i].wait_recv()
        spread(i)
    lax.fori_loop(KV // 2, KV, attend, 0)
    y_att = []
    for i, d in enumerate((1, 3, 2)):
        pair = pl.ds(((y + d) % NY) * 2, 2)
        y_att.append(
            (
                remote(ys_buf.at[pair], ysr_buf.at[i], y_send.at[0, i], y_recv.at[0, i], at_y(d)),
                remote(ya_buf.at[pair], yar_buf.at[i], y_send.at[1, i], y_recv.at[1, i], at_y(d)),
            )
        )
        for copy in y_att[-1]:
            copy.start()
    for i in (4, 5, 6, 7):
        windows[i].wait_recv()
        spread(i)
    for i in (0, 1, 2):
        pass_on(i)
    pl.semaphore_wait(hello.at[0], 1)
    pl.semaphore_wait(hello.at[1], 1)
    signal(hello.at[2], at_z(8))
    signal(hello.at[3], at_z(-8))

    for low in range(ZLO):
        there = (z + 28 + (low - z + 4 + NZ) % ZLO) % NZ
        lanes = (y * ZHI + there // ZLO) * 8
        r = lax.broadcasted_iota(jnp.int32, (128, 256), 0)
        c = lax.broadcasted_iota(jnp.int32, (128, 256), 1)
        k = c & 127
        hit = jnp.logical_and(
            jnp.logical_and((k >> 4) == low, ((k >> 3) & 1) == (c >> 7)), r == lanes + (k & 7)
        )
        sel_mat[low * 128 : (low + 1) * 128, :] = jnp.where(hit, 1.0, 0.0).astype(BF16)
    loads[7].wait()
    xp.wait_recv()
    for other in range(NX):
        columns = pl.ds(pl.multiple_of((g * NX + other) * 1024, 1024), 1024)
        for s in range(STEPS):
            xf_buf[other * 32 + 4 * s : other * 32 + 4 * s + 4] = x4_buf[s, :, columns].astype(F32)
            xf_buf[other * 32 + 16 + 4 * s : other * 32 + 16 + 4 * s + 4] = xp_buf[
                s, :, other * 1024 : (other + 1) * 1024
            ].astype(F32)
    pick_buf[...] = jnp.dot(xf_buf[...].astype(BF16), sel_mat[...], preferred_element_type=F32)

    def slab_product(owner):
        lhs = pick_buf[pl.ds(pl.multiple_of(owner * 32, 32), 32), :].astype(BF16)
        lhs = jnp.concatenate([lhs[:, :128], lhs[:, 128:]], axis=0)
        slab = w_buf[owner]
        top = jnp.max(jnp.abs(slab.astype(F32)), axis=0)
        return jnp.dot(lhs, slab.reshape(128, 512), preferred_element_type=F32), top

    partial, top = slab_product(x)
    for i in (3, 4, 5):
        pass_on(i)

    for copies in y_att:
        for copy in copies:
            copy.wait_recv()
    for pair in range(2):
        stats = [ys_buf[y * 2 + pair]] + [ysr_buf[i, pair] for i in range(3)]
        parts = [ya_buf[y * 2 + pair]] + [yar_buf[i, pair] for i in range(3)]
        peak = functools.reduce(jnp.maximum, [s[0:1] for s in stats])
        factors = [jnp.exp(s[0:1] - peak) for s in stats]
        total = sum(s[1:2] * f for s, f in zip(stats, factors))
        part = sum(p.astype(F32) * f for p, f in zip(parts, factors))
        zs_buf[pair] = jnp.concatenate([peak, total], axis=0)
        turned = part.T.astype(BF16)
        za_buf[2 * pair] = turned[:64]
        za_buf[2 * pair + 1] = turned[64:]
    pl.semaphore_wait(hello.at[2], 1)
    pl.semaphore_wait(hello.at[3], 1)
    z_att = []
    for i, d in enumerate((2, 1, 3)):
        dest = (zh + d) % ZHI
        z_att.append(
            (
                remote(zs_buf.at[dest // 2], zsr_buf.at[i], z_send.at[0, i], z_recv.at[0, i], at_z(8 * d)),
                remote(za_buf.at[dest], zar_buf.at[i], z_send.at[1, i], z_recv.at[1, i], at_z(8 * d)),
            )
        )
        for copy in z_att[-1]:
            copy.start()

    for i in (6, 7):
        pass_on(i)
    for owner in (left, right):
        more, more_top = slab_product(owner)
        partial, top = partial + more, jnp.maximum(top, more_top)
    for i in range(8):
        from_across[i].wait_recv()
    more, more_top = slab_product(across)
    partial, top = partial + more, jnp.maximum(top, more_top)

    tops = [
        jnp.broadcast_to(jnp.max(top[h * 8 : h * 8 + 8], axis=0, keepdims=True), (8, 512))
        for h in range(2)
    ]
    for h in range(2):
        cs_buf[h, 0:16] = partial[h * 32 + 16 : h * 32 + 32]
        cs_buf[h, 16:24] = tops[h]
    core = remote(cs_buf, cr_buf, c_sem.at[0], c_sem.at[1], partner)
    core.start()
    core.wait_recv()
    for h in range(2):
        both = partial[h * 32 : h * 32 + 16] + cr_buf[h, 0:16]
        highest = jnp.maximum(tops[h], cr_buf[h, 16:24])
        for k in range(2):
            yf_buf[2 * h + k, 0:16] = both[:, k * 256 : (k + 1) * 256]
            yf_buf[2 * h + k, 16:24] = highest[:, k * 256 : (k + 1) * 256]
    y_new = []
    for i, d in enumerate((1, 3, 2)):
        copy = remote(yf_buf.at[(y + d) % NY], yfr_buf.at[i], y_send.at[2, i], y_recv.at[2, i], at_y(d))
        copy.start()
        y_new.append(copy)
    for copy in y_new:
        copy.wait_recv()
    blocks = [yf_buf[y]] + [yfr_buf[i] for i in range(3)]
    added = sum(b[0:16] for b in blocks)
    highest = functools.reduce(jnp.maximum, [b[16:17] for b in blocks])
    for k in range(2):
        zf_buf[k] = added[:, k * 128 : (k + 1) * 128].astype(BF16)
        zm_buf[k] = highest[:, k * 128 : (k + 1) * 128]
    z_new = []
    for i, d in enumerate((2, 1, 3)):
        dest = (zh + d) % ZHI
        z_new.append(
            (
                remote(zf_buf.at[dest // 2], zfr_buf.at[i], z_send.at[2, i], z_recv.at[2, i], at_z(8 * d)),
                remote(zm_buf.at[dest // 2], zmr_buf.at[i], z_send.at[3, i], z_recv.at[3, i], at_z(8 * d)),
            )
        )
        for copy in z_new[-1]:
            copy.start()
    mine = jnp.where((zh // 2) == 1, added[:, 128:], added[:, :128])

    head = y * 2 + zh // 2
    loads[8].wait()
    own_keys = jnp.concatenate(
        [nk4_buf[s, :, pl.ds(pl.multiple_of(head * 128, 128), 128)].astype(F32) for s in range(STEPS)], axis=0
    ).astype(BF16)
    new_scores = (
        lax.dot_general(own_keys, head_queries(head), (((1,), (1,)), ((), ())), preferred_element_type=F32)
        * inverse
    )
    r = lax.broadcasted_iota(jnp.int32, (16, 128), 0)
    c = lax.broadcasted_iota(jnp.int32, (16, 128), 1)
    causal = jnp.logical_and((r & 3) == (c & 3), (r >> 2) <= ((c >> 2) & 3))
    new_scores = jnp.where(causal, new_scores, masked_score)
    new_peak = jnp.max(new_scores, axis=0, keepdims=True)

    for copies in z_att:
        for copy in copies:
            copy.wait_recv()
    stats = [zs_buf[zh // 2]] + [zsr_buf[i] for i in range(3)]
    parts = [za_buf[zh]] + [zar_buf[i] for i in range(3)]
    peak = functools.reduce(jnp.maximum, [s[0:1] for s in stats] + [new_peak])
    factors = [jnp.exp(s[0:1] - peak) for s in stats]
    new_weights = jnp.where(causal, jnp.exp(new_scores - peak), 0.0)
    denominator = sum(s[1:2] * f for s, f in zip(stats, factors)) + jnp.sum(
        new_weights, axis=0, keepdims=True
    )
    share = 1.0 / denominator
    columns = jnp.concatenate([f * share for f in factors] + [share] * 4, axis=0).T
    odd = (zh % 2) == 1
    columns = jnp.where(odd, columns[64:], columns[:64])
    merged = sum(p.astype(F32) * columns[:, i : i + 1] for i, p in enumerate(parts))

    for copies in z_new:
        for copy in copies:
            copy.wait_recv()
    values = (mine + sum(zfr_buf[i].astype(F32) for i in range(3))).astype(BF16)
    highest = functools.reduce(jnp.maximum, [zm_buf[zh // 2]] + [zmr_buf[i] for i in range(3)])
    scales = (highest + scale_floor) / code_range
    scale_ref[...] = jnp.broadcast_to(jnp.where(odd, scales[:, 64:], scales[:, :64]), (8, 64))
    wide = values.astype(F32)
    fresh_ref[...] = jnp.where(odd, wide[:, 64:], wide[:, :64])
    mixed = lax.dot_general(
        new_weights.astype(BF16), values, (((0,), (0,)), ((), ())), preferred_element_type=F32
    )
    mixed = jnp.where(odd, mixed[64:], mixed[:64])
    result = merged + mixed * columns[:, 4:5]
    for h in range(4):
        att_ref[:, h * 128 : (h + 1) * 128] = result[h * 16 : (h + 1) * 16]

    for copy in windows[1:] + [xp, core] + y_new:
        copy.wait_send()
    for i in range(8):
        from_left[i].wait_send()
        from_right[i].wait_send()
        from_across[i].wait_send()
    for copies in y_att + z_att + z_new:
        for copy in copies:
            copy.wait_send()


def finish(mw, grad, m1, m2, step, scale, fresh, att, nw_out, scale_out, fresh_out, att_out):
    nw_out[...] = adamw(mw[...], grad[...], m1[...], m2[...], step[0])
    scale_out[...] = scale[0:1]
    for s in range(STEPS):
        fresh_out[s] = fresh[4 * s : 4 * s + 4].astype(BF16)
        att_out[s] = att[4 * s : 4 * s + 4]


def body(
    master_weight,
    grad,
    moment1,
    moment2,
    step_count,
    x_new,
    queries,
    new_keys,
    cache_keys,
    cache_values,
    lengths,
):
    vmem = pl.BlockSpec(memory_space=pltpu.VMEM)
    smem = pl.BlockSpec(memory_space=pltpu.SMEM)
    hbm = pl.BlockSpec(memory_space=pl.ANY)
    dma = pltpu.SemaphoreType.DMA
    optimizer = (master_weight, grad, moment1, moment2, step_count)
    scale, fresh, attention = pl.pallas_call(
        kernel,
        out_shape=(
            jax.ShapeDtypeStruct((8, 64), F32),
            jax.ShapeDtypeStruct((16, 64), F32),
            jax.ShapeDtypeStruct((16, 512), F32),
        ),
        in_specs=[hbm] * 4 + [smem] + [hbm] * 5 + [smem],
        out_specs=(vmem,) * 3,
        scratch_shapes=[
            pltpu.VMEM((4, 8, 1024), F32),
            pltpu.VMEM((STEPS, BR, 8192), BF16),
            pltpu.VMEM((STEPS, BR, 8192), BF16),
            pltpu.VMEM((STEPS, BR, 1024), BF16),
            pltpu.VMEM((256, 1024), BF16),
            pltpu.VMEM((256, 1024), BF16),
            pltpu.VMEM((128, 1024), F32),
            pltpu.VMEM((16, 8192), F32),
            pltpu.VMEM((NX, ZLO, 16, 512), BF16),
            pltpu.VMEM((STEPS, BR, 4096), BF16),
            pltpu.VMEM((1024, 256), BF16),
            pltpu.VMEM((128, 256), F32),
            pltpu.VMEM((256, 128), F32),
            pltpu.VMEM((KV, 128, 128), BF16),
            pltpu.VMEM((KV, 2, 128), F32),
            pltpu.VMEM((3, 2, 128, 128), BF16),
            pltpu.VMEM((3, 2, 2, 128), F32),
            pltpu.VMEM((4, 64, 128), BF16),
            pltpu.VMEM((2, 2, 128), F32),
            pltpu.VMEM((3, 64, 128), BF16),
            pltpu.VMEM((3, 2, 128), F32),
            pltpu.VMEM((2, 24, 512), F32),
            pltpu.VMEM((2, 24, 512), F32),
            pltpu.VMEM((4, 24, 256), F32),
            pltpu.VMEM((3, 24, 256), F32),
            pltpu.VMEM((2, 16, 128), BF16),
            pltpu.VMEM((3, 16, 128), BF16),
            pltpu.VMEM((2, 1, 128), F32),
            pltpu.VMEM((3, 1, 128), F32),
            dma((9,)),
            dma((8,)),
            dma((8,)),
            dma((3, 8)),
            dma((3, 8)),
            dma((2,)),
            dma((2,)),
            dma((3, 3)),
            dma((3, 3)),
            dma((4, 3)),
            dma((4, 3)),
            pltpu.SemaphoreType.REGULAR((4,)),
        ],
        compiler_params=pltpu.CompilerParams(collective_id=0, has_side_effects=True),
    )(
        *optimizer,
        x_new,
        queries,
        new_keys,
        cache_keys.reshape(256, 1024),
        cache_values.reshape(256, 1024),
        lengths,
    )
    new_weight, scale, fresh, attention = pl.pallas_call(
        finish,
        out_shape=(
            jax.ShapeDtypeStruct((8, 1024), F32),
            jax.ShapeDtypeStruct((1, 64), F32),
            jax.ShapeDtypeStruct((STEPS, BR, 64), BF16),
            jax.ShapeDtypeStruct((STEPS, BR, 512), F32),
        ),
        in_specs=[vmem] * 4 + [smem] + [vmem] * 3,
        out_specs=(vmem,) * 4,
    )(*optimizer, scale, fresh, attention)
    return new_weight, scale[0], fresh, attention


def solution(mesh):
    return jax.shard_map(
        body,
        mesh=mesh,
        in_specs=(
            P(("group", "rep", "tp"), None),
            P(("group", "rep", "tp"), None),
            P(("group", "rep", "tp"), None),
            P(("group", "rep", "tp"), None),
            P(),
            P(None, ("group", "rep"), None),
            P(None, ("group", "rep"), None),
            P(None, ("group", "rep"), None),
            P(("group", "rep"), "tp", None),
            P(("group", "rep"), "tp", None),
            P(("group", "rep"), None),
        ),
        out_specs=(
            P(("group", "rep", "tp"), None),
            P("tp"),
            P(None, ("group", "rep"), "tp"),
            P(None, ("group", "rep"), "tp"),
        ),
        check_vma=False,
    )
```

```python
import functools
import math

import jax
import jax.numpy as jnp
from jax import lax
from jax.experimental import pallas as pl
from jax.experimental.pallas import tpu as pltpu
from jax.sharding import PartitionSpec as P

H = 64
KV = 8
HD = 128
STEPS = 4
BR = 4

beta_first = 0.9
beta_second = 0.999
learn_rate = 0.01
decay_rate = 0.1
adam_floor = 1e-08
scale_floor = 1e-06
code_range = 448.0
masked_score = -1e30

F32 = jnp.float32
BF16 = jnp.bfloat16
MESH = pl.DeviceIdType.MESH

NX, NY, ZLO, ZHI = 4, 4, 8, 4
NZ = ZLO * ZHI
SOURCES = (0, -1, 1, -2, 2, -3, 3, -4)
NEAR = tuple(
    (dx, dy, dg)
    for far in (4, 3, 2, 1, 0)
    for dx in range(NX)
    for dy in range(NY)
    for dg in range(2)
    if min(dx, NX - dx) + min(dy, NY - dy) == far and (dx, dy, dg) != (0, 0, 0)
)


def adamw(mw, grad, m1, m2, step):
    steps_done = jnp.full(mw.shape, step, jnp.int32).astype(F32)
    first = beta_first * m1 + (1.0 - beta_first) * grad
    second = beta_second * m2 + (1.0 - beta_second) * grad * grad
    correction = jnp.sqrt(1.0 - jnp.exp(steps_done * math.log(beta_second))) / (
        1.0 - jnp.exp(steps_done * math.log(beta_first))
    )
    return mw - learn_rate * correction * first / (jnp.sqrt(second) + adam_floor) - learn_rate * decay_rate * mw


def kernel(
    mw_hbm,
    grad_hbm,
    m1_hbm,
    m2_hbm,
    step_ref,
    x_hbm,
    q_hbm,
    nk_hbm,
    k_hbm,
    v_hbm,
    len_ref,
    scale_ref,
    fresh_ref,
    att_ref,
    rows_buf,
    x4_buf,
    q4_buf,
    nk4_buf,
    k_ref,
    v_ref,
    xf_buf,
    q_ref,
    w_buf,
    sel_mat,
    ps_buf,
    pr_buf,
    mask_buf,
    ya_buf,
    ys_buf,
    yar_buf,
    ysr_buf,
    za_buf,
    zs_buf,
    zar_buf,
    zsr_buf,
    pd_buf,
    pdr_buf,
    pm_buf,
    pmr_buf,
    zf_buf,
    zfr_buf,
    zm_buf,
    zmr_buf,
    in_sem,
    win_send,
    win_recv,
    pick_send,
    pick_recv,
    d_send,
    d_recv,
    m_send,
    m_recv,
    y_send,
    y_recv,
    z_send,
    z_recv,
    hello,
):
    g = lax.axis_index("group")
    rep = lax.axis_index("rep")
    tp = lax.axis_index("tp")
    x, zl = rep // ZLO, rep % ZLO
    y, zh = tp // ZHI, tp % ZHI
    z = zh * ZLO + zl

    def at_z(offset):
        there = (z + offset + NZ) % NZ
        return {"rep": x * ZLO + there % ZLO, "tp": y * ZHI + there // ZLO}

    def at_y(offset):
        return {"tp": ((y + offset) % NY) * ZHI + zh}

    def at_xyg(dx, dy, dg):
        return {
            "group": 1 - g if dg else g,
            "rep": ((x + dx) % NX) * ZLO + zl,
            "tp": ((y + dy) % NY) * ZHI + zh,
        }

    def signal(sem, peer):
        pl.semaphore_signal(sem, inc=1, device_id=peer, device_id_type=MESH)

    def remote(src, dst, send, recv, peer):
        return pltpu.make_async_remote_copy(
            src_ref=src, dst_ref=dst, send_sem=send, recv_sem=recv, device_id=peer, device_id_type=MESH
        )

    barrier = pltpu.get_barrier_semaphore()
    peers = [at_z(d) for d in (4, -4, 3, -3, 2, -2, 1, -1)]
    peers += [at_xyg(*there) for there in NEAR]
    for peer in peers:
        signal(barrier, peer)

    loads = [
        pltpu.make_async_copy(src, dst, in_sem.at[i])
        for i, (src, dst) in enumerate(
            [(ref, rows_buf.at[i]) for i, ref in enumerate((mw_hbm, grad_hbm, m1_hbm, m2_hbm))]
            + [(q_hbm, q4_buf), (k_hbm, k_ref), (v_hbm, v_ref), (x_hbm, x4_buf), (nk_hbm, nk4_buf)]
        )
    ]
    for copy in loads:
        copy.start()

    for low in range(ZLO):
        there = (z + 28 + (low - z + 4 + NZ) % ZLO) % NZ
        lanes = (y * ZHI + there // ZLO) * 8
        r = lax.broadcasted_iota(jnp.int32, (128, 256), 0)
        c = lax.broadcasted_iota(jnp.int32, (128, 256), 1)
        k = c & 127
        hit = jnp.logical_and(
            jnp.logical_and((k >> 4) == low, ((k >> 3) & 1) == (c >> 7)), r == lanes + (k & 7)
        )
        sel_mat[low * 128 : (low + 1) * 128, :] = jnp.where(hit, 1.0, 0.0).astype(BF16)

    for copy in loads[:4]:
        copy.wait()
    nw = adamw(rows_buf[0], rows_buf[1], rows_buf[2], rows_buf[3], step_ref[0])
    w_buf[zl] = jnp.concatenate([nw[:, :512], nw[:, 512:]], axis=0).astype(BF16)

    pl.semaphore_wait(barrier, len(peers))

    windows = [None]
    for i, e in enumerate(SOURCES):
        if e:
            own = w_buf.at[zl]
            copy = remote(own, own, win_send.at[i], win_recv.at[i], at_z(-e))
            copy.start()
            windows.append(copy)
    loads[7].wait()
    for j in range(8):
        for step in range(STEPS):
            xf_buf[j * 16 + 4 * step : j * 16 + 4 * step + 4] = x4_buf[
                step, :, j * 1024 : (j + 1) * 1024
            ].astype(F32)
    picked = jnp.dot(xf_buf[...].astype(BF16), sel_mat[...], preferred_element_type=F32).astype(BF16)
    for j in range(8):
        ps_buf[j] = picked[j * 16 : (j + 1) * 16]
    picks = []
    for dx, dg in ((2, 1), (2, 0), (1, 1), (1, 0), (3, 1), (3, 0), (0, 1)):
        there = (1 - g if dg else g) * NX + (x + dx) % NX
        back = ((NX - dx) % NX) * 2 + dg
        copy = remote(
            ps_buf.at[there], pr_buf.at[back], pick_send.at[back], pick_recv.at[back], at_xyg(dx, 0, dg)
        )
        copy.start()
        picks.append(copy)
    signal(hello.at[0], at_z(4))
    signal(hello.at[1], at_z(-4))

    rows_b = []
    lane_b = lax.broadcasted_iota(jnp.int32, (64, 128), 1) & 3
    position = tp * 64 + lax.broadcasted_iota(jnp.int32, (64, 128), 0)
    for b in range(BR):
        live = jnp.logical_and(position < len_ref[0, b], lane_b == b)
        rows_b.append(jnp.where(live, 1.0, 0.0))
    mask_buf[...] = jnp.concatenate(rows_b, axis=0)
    inverse = 1.0 / math.sqrt(HD)
    loads[4].wait()
    for s in range(STEPS):
        q_ref[4 * s : 4 * s + 4] = q4_buf[s].astype(F32)

    def head_queries(kv):
        return jnp.concatenate(
            [q_ref[:, pl.ds(pl.multiple_of(kv * 1024 + h * 128, 128), 128)] for h in range(8)], axis=0
        ).astype(BF16)

    def attend(kv, carry):
        columns = pl.ds(pl.multiple_of(kv * 128, 128), 128)
        scores = (
            lax.dot_general(
                k_ref[:, columns], head_queries(kv), (((1,), (1,)), ((), ())), preferred_element_type=F32
            )
            * inverse
        )
        live = mask_buf[...] > 0.5
        masked = jnp.where(live, scores, masked_score)
        peak = jnp.max(masked, axis=0, keepdims=True)
        weights = jnp.where(live, jnp.exp(masked - peak), 0.0)
        total = jnp.sum(weights, axis=0, keepdims=True)
        part = lax.dot_general(
            v_ref[:, columns],
            weights.astype(BF16),
            (((0,), (0,)), ((), ())),
            preferred_element_type=F32,
        )
        ya_buf[kv] = part.astype(BF16)
        ys_buf[kv] = jnp.concatenate([peak, total], axis=0)
        return carry

    loads[5].wait()
    loads[6].wait()
    lax.fori_loop(0, KV, attend, 0)
    y_att = []
    for i, d in enumerate((1, 3, 2)):
        pair = pl.ds(((y + d) % NY) * 2, 2)
        y_att.append(
            (
                remote(ys_buf.at[pair], ysr_buf.at[i], y_send.at[0, i], y_recv.at[0, i], at_y(d)),
                remote(ya_buf.at[pair], yar_buf.at[i], y_send.at[1, i], y_recv.at[1, i], at_y(d)),
            )
        )
        for copy in y_att[-1]:
            copy.start()
    for copy in picks:
        copy.wait_recv()
    lhs = jnp.concatenate([ps_buf[g * NX + x]] + [pr_buf[i] for i in range(1, 8)], axis=0)
    lhs = jnp.concatenate([lhs[:, :128], lhs[:, 128:]], axis=0)
    for copy in windows[1:]:
        copy.wait_recv()
    rows = w_buf[...]
    product = jnp.dot(lhs, rows.reshape(128, 512), preferred_element_type=F32).astype(BF16)
    top = jnp.max(jnp.abs(rows.astype(F32)), axis=0)
    for h in range(2):
        high = jnp.max(top[h * 8 : h * 8 + 8], axis=0, keepdims=True)
        for k in range(2):
            pm_buf[2 * h + k] = high[:, k * 256 : (k + 1) * 256]
            for i in range(8):
                first = h * 128 + i * 16
                pd_buf[i, 2 * h + k] = product[first : first + 16, k * 256 : (k + 1) * 256]
    direct = []
    for dx, dy, dg in NEAR:
        there = (y + dy) % NY
        back = (((NX - dx) % NX) * NY + (NY - dy) % NY) * 2 + dg
        peer = at_xyg(dx, dy, dg)
        direct += [
            remote(pd_buf.at[dx * 2 + dg, there], pdr_buf.at[back], d_send.at[back], d_recv.at[back], peer),
            remote(pm_buf.at[there], pmr_buf.at[back], m_send.at[back], m_recv.at[back], peer),
        ]
        direct[-2].start()
        direct[-1].start()
    pl.semaphore_wait(hello.at[0], 1)
    pl.semaphore_wait(hello.at[1], 1)
    signal(hello.at[2], at_z(8))
    signal(hello.at[3], at_z(-8))

    for copies in y_att:
        for copy in copies:
            copy.wait_recv()
    for pair in range(2):
        stats = [ys_buf[y * 2 + pair]] + [ysr_buf[i, pair] for i in range(3)]
        parts = [ya_buf[y * 2 + pair]] + [yar_buf[i, pair] for i in range(3)]
        peak = functools.reduce(jnp.maximum, [s[0:1] for s in stats])
        factors = [jnp.exp(s[0:1] - peak) for s in stats]
        total = sum(s[1:2] * f for s, f in zip(stats, factors))
        part = sum(p.astype(F32) * f for p, f in zip(parts, factors))
        zs_buf[pair] = jnp.concatenate([peak, total], axis=0)
        turned = part.T.astype(BF16)
        za_buf[2 * pair] = turned[:64]
        za_buf[2 * pair + 1] = turned[64:]
    pl.semaphore_wait(hello.at[2], 1)
    pl.semaphore_wait(hello.at[3], 1)
    z_att = []
    for i, d in enumerate((2, 1, 3)):
        dest = (zh + d) % ZHI
        z_att.append(
            (
                remote(zs_buf.at[dest // 2], zsr_buf.at[i], z_send.at[0, i], z_recv.at[0, i], at_z(8 * d)),
                remote(za_buf.at[dest], zar_buf.at[i], z_send.at[1, i], z_recv.at[1, i], at_z(8 * d)),
            )
        )
        for copy in z_att[-1]:
            copy.start()

    for copy in direct:
        copy.wait_recv()
    added = pd_buf[0, y].astype(F32) + sum(pdr_buf[i].astype(F32) for i in range(1, 32))
    highest = functools.reduce(jnp.maximum, [pm_buf[y]] + [pmr_buf[i] for i in range(1, 32)])
    for k in range(2):
        zf_buf[k] = added[:, k * 128 : (k + 1) * 128].astype(BF16)
        zm_buf[k] = highest[:, k * 128 : (k + 1) * 128]
    z_new = []
    for i, d in enumerate((2, 1, 3)):
        dest = (zh + d) % ZHI
        z_new.append(
            (
                remote(zf_buf.at[dest // 2], zfr_buf.at[i], z_send.at[2, i], z_recv.at[2, i], at_z(8 * d)),
                remote(zm_buf.at[dest // 2], zmr_buf.at[i], z_send.at[3, i], z_recv.at[3, i], at_z(8 * d)),
            )
        )
        for copy in z_new[-1]:
            copy.start()
    mine = jnp.where((zh // 2) == 1, added[:, 128:], added[:, :128])

    head = y * 2 + zh // 2
    loads[8].wait()
    own_keys = jnp.concatenate(
        [nk4_buf[s, :, pl.ds(pl.multiple_of(head * 128, 128), 128)].astype(F32) for s in range(STEPS)], axis=0
    ).astype(BF16)
    new_scores = (
        lax.dot_general(own_keys, head_queries(head), (((1,), (1,)), ((), ())), preferred_element_type=F32)
        * inverse
    )
    r = lax.broadcasted_iota(jnp.int32, (16, 128), 0)
    c = lax.broadcasted_iota(jnp.int32, (16, 128), 1)
    causal = jnp.logical_and((r & 3) == (c & 3), (r >> 2) <= ((c >> 2) & 3))
    new_scores = jnp.where(causal, new_scores, masked_score)
    new_peak = jnp.max(new_scores, axis=0, keepdims=True)

    for copies in z_att:
        for copy in copies:
            copy.wait_recv()
    stats = [zs_buf[zh // 2]] + [zsr_buf[i] for i in range(3)]
    parts = [za_buf[zh]] + [zar_buf[i] for i in range(3)]
    peak = functools.reduce(jnp.maximum, [s[0:1] for s in stats] + [new_peak])
    factors = [jnp.exp(s[0:1] - peak) for s in stats]
    new_weights = jnp.where(causal, jnp.exp(new_scores - peak), 0.0)
    denominator = sum(s[1:2] * f for s, f in zip(stats, factors)) + jnp.sum(
        new_weights, axis=0, keepdims=True
    )
    share = 1.0 / denominator
    columns = jnp.concatenate([f * share for f in factors] + [share] * 4, axis=0).T
    odd = (zh % 2) == 1
    columns = jnp.where(odd, columns[64:], columns[:64])
    merged = sum(p.astype(F32) * columns[:, i : i + 1] for i, p in enumerate(parts))

    for copies in z_new:
        for copy in copies:
            copy.wait_recv()
    values = (mine + sum(zfr_buf[i].astype(F32) for i in range(3))).astype(BF16)
    highest = functools.reduce(jnp.maximum, [zm_buf[zh // 2]] + [zmr_buf[i] for i in range(3)])
    scales = (highest + scale_floor) / code_range
    scale_ref[...] = jnp.broadcast_to(jnp.where(odd, scales[:, 64:], scales[:, :64]), (8, 64))
    wide = values.astype(F32)
    fresh_ref[...] = jnp.where(odd, wide[:, 64:], wide[:, :64])
    mixed = lax.dot_general(
        new_weights.astype(BF16), values, (((0,), (0,)), ((), ())), preferred_element_type=F32
    )
    mixed = jnp.where(odd, mixed[64:], mixed[:64])
    result = merged + mixed * columns[:, 4:5]
    for h in range(4):
        att_ref[:, h * 128 : (h + 1) * 128] = result[h * 16 : (h + 1) * 16]

    for copy in windows[1:] + picks + direct:
        copy.wait_send()
    for copies in y_att + z_att + z_new:
        for copy in copies:
            copy.wait_send()


def finish(mw, grad, m1, m2, step, scale, fresh, att, nw_out, scale_out, fresh_out, att_out):
    nw_out[...] = adamw(mw[...], grad[...], m1[...], m2[...], step[0])
    scale_out[...] = scale[0:1]
    for s in range(STEPS):
        fresh_out[s] = fresh[4 * s : 4 * s + 4].astype(BF16)
        att_out[s] = att[4 * s : 4 * s + 4]


def body(
    master_weight,
    grad,
    moment1,
    moment2,
    step_count,
    x_new,
    queries,
    new_keys,
    cache_keys,
    cache_values,
    lengths,
):
    vmem = pl.BlockSpec(memory_space=pltpu.VMEM)
    smem = pl.BlockSpec(memory_space=pltpu.SMEM)
    hbm = pl.BlockSpec(memory_space=pl.ANY)
    dma = pltpu.SemaphoreType.DMA
    optimizer = (master_weight, grad, moment1, moment2, step_count)
    scale, fresh, attention = pl.pallas_call(
        kernel,
        out_shape=(
            jax.ShapeDtypeStruct((8, 64), F32),
            jax.ShapeDtypeStruct((16, 64), F32),
            jax.ShapeDtypeStruct((16, 512), F32),
        ),
        in_specs=[hbm] * 4 + [smem] + [hbm] * 5 + [smem],
        out_specs=(vmem,) * 3,
        scratch_shapes=[
            pltpu.VMEM((4, 8, 1024), F32),
            pltpu.VMEM((STEPS, BR, 8192), BF16),
            pltpu.VMEM((STEPS, BR, 8192), BF16),
            pltpu.VMEM((STEPS, BR, 1024), BF16),
            pltpu.VMEM((256, 1024), BF16),
            pltpu.VMEM((256, 1024), BF16),
            pltpu.VMEM((128, 1024), F32),
            pltpu.VMEM((16, 8192), F32),
            pltpu.VMEM((ZLO, 16, 512), BF16),
            pltpu.VMEM((1024, 256), BF16),
            pltpu.VMEM((8, 16, 256), BF16),
            pltpu.VMEM((8, 16, 256), BF16),
            pltpu.VMEM((256, 128), F32),
            pltpu.VMEM((KV, 128, 128), BF16),
            pltpu.VMEM((KV, 2, 128), F32),
            pltpu.VMEM((3, 2, 128, 128), BF16),
            pltpu.VMEM((3, 2, 2, 128), F32),
            pltpu.VMEM((4, 64, 128), BF16),
            pltpu.VMEM((2, 2, 128), F32),
            pltpu.VMEM((3, 64, 128), BF16),
            pltpu.VMEM((3, 2, 128), F32),
            pltpu.VMEM((8, NY, 16, 256), BF16),
            pltpu.VMEM((32, 16, 256), BF16),
            pltpu.VMEM((NY, 1, 256), F32),
            pltpu.VMEM((32, 1, 256), F32),
            pltpu.VMEM((2, 16, 128), BF16),
            pltpu.VMEM((3, 16, 128), BF16),
            pltpu.VMEM((2, 1, 128), F32),
            pltpu.VMEM((3, 1, 128), F32),
            dma((9,)),
            dma((8,)),
            dma((8,)),
            dma((8,)),
            dma((8,)),
            dma((32,)),
            dma((32,)),
            dma((32,)),
            dma((32,)),
            dma((3, 3)),
            dma((3, 3)),
            dma((4, 3)),
            dma((4, 3)),
            pltpu.SemaphoreType.REGULAR((4,)),
        ],
        compiler_params=pltpu.CompilerParams(collective_id=0, has_side_effects=True),
    )(
        *optimizer,
        x_new,
        queries,
        new_keys,
        cache_keys.reshape(256, 1024),
        cache_values.reshape(256, 1024),
        lengths,
    )
    new_weight, scale, fresh, attention = pl.pallas_call(
        finish,
        out_shape=(
            jax.ShapeDtypeStruct((8, 1024), F32),
            jax.ShapeDtypeStruct((1, 64), F32),
            jax.ShapeDtypeStruct((STEPS, BR, 64), BF16),
            jax.ShapeDtypeStruct((STEPS, BR, 512), F32),
        ),
        in_specs=[vmem] * 4 + [smem] + [vmem] * 3,
        out_specs=(vmem,) * 4,
    )(*optimizer, scale, fresh, attention)
    return new_weight, scale[0], fresh, attention


def solution(mesh):
    return jax.shard_map(
        body,
        mesh=mesh,
        in_specs=(
            P(("group", "rep", "tp"), None),
            P(("group", "rep", "tp"), None),
            P(("group", "rep", "tp"), None),
            P(("group", "rep", "tp"), None),
            P(),
            P(None, ("group", "rep"), None),
            P(None, ("group", "rep"), None),
            P(None, ("group", "rep"), None),
            P(("group", "rep"), "tp", None),
            P(("group", "rep"), "tp", None),
            P(("group", "rep"), None),
        ),
        out_specs=(
            P(("group", "rep", "tp"), None),
            P("tp"),
            P(None, ("group", "rep"), "tp"),
            P(None, ("group", "rep"), "tp"),
        ),
        check_vma=False,
    )
```

```python
import functools
import math

import jax
import jax.numpy as jnp
from jax import lax
from jax.experimental import pallas as pl
from jax.experimental.pallas import tpu as pltpu
from jax.sharding import PartitionSpec as P

H = 64
KV = 8
HD = 128
STEPS = 4
BR = 4

beta_first = 0.9
beta_second = 0.999
learn_rate = 0.01
decay_rate = 0.1
adam_floor = 1e-08
scale_floor = 1e-06
code_range = 448.0
masked_score = -1e30

F32 = jnp.float32
BF16 = jnp.bfloat16
MESH = pl.DeviceIdType.MESH

NX, NY, ZLO, ZHI = 4, 4, 8, 4
NZ = ZLO * ZHI
SOURCES = (-4, 3, -3, 2, -2, 1, -1)
NEAR = tuple(
    (dx, dy, dg)
    for far in (4, 3, 2, 1, 0)
    for dx in range(NX)
    for dy in range(NY)
    for dg in range(2)
    if min(dx, NX - dx) + min(dy, NY - dy) == far and (dx, dy, dg) != (0, 0, 0)
)


def adamw(mw, grad, m1, m2, step):
    steps_done = jnp.full(mw.shape, step, jnp.int32).astype(F32)
    first = beta_first * m1 + (1.0 - beta_first) * grad
    second = beta_second * m2 + (1.0 - beta_second) * grad * grad
    correction = jnp.sqrt(1.0 - jnp.exp(steps_done * math.log(beta_second))) / (
        1.0 - jnp.exp(steps_done * math.log(beta_first))
    )
    return mw - learn_rate * correction * first / (jnp.sqrt(second) + adam_floor) - learn_rate * decay_rate * mw


def kernel(
    mw_hbm,
    grad_hbm,
    m1_hbm,
    m2_hbm,
    step_ref,
    x_hbm,
    q_hbm,
    nk_hbm,
    k_hbm,
    v_hbm,
    len_ref,
    scale_ref,
    fresh_ref,
    att_ref,
    rows_buf,
    x4_buf,
    q4_buf,
    nk4_buf,
    k_ref,
    v_ref,
    xf_buf,
    q_ref,
    w_buf,
    sel_mat,
    ps_buf,
    pr_buf,
    mask_buf,
    ya_buf,
    ys_buf,
    yar_buf,
    ysr_buf,
    za_buf,
    zs_buf,
    zar_buf,
    zsr_buf,
    pd_buf,
    pdr_buf,
    pm_buf,
    pmr_buf,
    zf_buf,
    zfr_buf,
    zm_buf,
    zmr_buf,
    in_sem,
    win_send,
    win_recv,
    pick_send,
    pick_recv,
    d_send,
    d_recv,
    m_send,
    m_recv,
    y_send,
    y_recv,
    z_send,
    z_recv,
    n_send,
    n_recv,
    hello,
):
    g = lax.axis_index("group")
    rep = lax.axis_index("rep")
    tp = lax.axis_index("tp")
    x, zl = rep // ZLO, rep % ZLO
    y, zh = tp // ZHI, tp % ZHI
    z = zh * ZLO + zl

    def at_z(offset):
        there = (z + offset + NZ) % NZ
        return {"rep": x * ZLO + there % ZLO, "tp": y * ZHI + there // ZLO}

    def at_y(offset):
        return {"tp": ((y + offset) % NY) * ZHI + zh}

    def at_xyg(dx, dy, dg, dz=0):
        there = (z + dz + NZ) % NZ
        return {
            "group": 1 - g if dg else g,
            "rep": ((x + dx) % NX) * ZLO + there % ZLO,
            "tp": ((y + dy) % NY) * ZHI + there // ZLO,
        }

    def signal(sem, peer):
        pl.semaphore_signal(sem, inc=1, device_id=peer, device_id_type=MESH)

    def remote(src, dst, send, recv, peer):
        return pltpu.make_async_remote_copy(
            src_ref=src, dst_ref=dst, send_sem=send, recv_sem=recv, device_id=peer, device_id_type=MESH
        )

    barrier = pltpu.get_barrier_semaphore()
    peers = [at_z(d) for d in (4, -4, 3, -3, 2, -2, 1, -1)]
    peers += [at_xyg(dx, 0, dg, dz) for dz in (4, -4) for dx in range(NX) for dg in range(2) if dx or dg]
    peers += [at_xyg(*there) for there in NEAR]
    for peer in peers:
        signal(barrier, peer)

    loads = [
        pltpu.make_async_copy(src, dst, in_sem.at[i])
        for i, (src, dst) in enumerate(
            [(ref, rows_buf.at[i]) for i, ref in enumerate((mw_hbm, grad_hbm, m1_hbm, m2_hbm))]
            + [(q_hbm, q4_buf), (k_hbm, k_ref), (v_hbm, v_ref), (x_hbm, x4_buf), (nk_hbm, nk4_buf)]
        )
    ]
    for copy in loads:
        copy.start()

    for low in range(ZLO):
        r = lax.broadcasted_iota(jnp.int32, (128, 128), 0)
        k = lax.broadcasted_iota(jnp.int32, (128, 128), 1)
        for way in range(2):
            base = z + (0 if way == 0 else NZ - 8)
            there = (base + (low - base + 2 * NZ) % ZLO) % NZ
            lanes = (y * ZHI + there // ZLO) * 8
            hit = jnp.logical_and((k >> 4) == low, r == lanes + (k & 7))
            sel_mat[low * 128 : (low + 1) * 128, way * 128 : (way + 1) * 128] = jnp.where(
                hit, 1.0, 0.0
            ).astype(BF16)

    for copy in loads[:4]:
        copy.wait()
    nw = adamw(rows_buf[0], rows_buf[1], rows_buf[2], rows_buf[3], step_ref[0])
    w_buf[zl] = jnp.concatenate([nw[:, :512], nw[:, 512:]], axis=0).astype(BF16)

    pl.semaphore_wait(barrier, len(peers))

    signal(hello.at[0], at_z(4))
    signal(hello.at[1], at_z(-4))
    windows = []
    for i, e in enumerate(SOURCES):
        own = w_buf.at[zl]
        copy = remote(own, own, win_send.at[i], win_recv.at[i], at_z(-e))
        copy.start()
        windows.append(copy)
    loads[7].wait()
    for j in range(8):
        for step in range(STEPS):
            xf_buf[j * 16 + 4 * step : j * 16 + 4 * step + 4] = x4_buf[
                step, :, j * 1024 : (j + 1) * 1024
            ].astype(F32)
    picked = jnp.dot(xf_buf[...].astype(BF16), sel_mat[...], preferred_element_type=F32).astype(BF16)
    for j in range(8):
        for way in range(2):
            ps_buf[way, j] = picked[j * 16 : (j + 1) * 16, way * 128 : (way + 1) * 128]
    picks = []
    for dx, dg in ((2, 0), (2, 1), (1, 0), (1, 1), (3, 0), (3, 1), (0, 0), (0, 1)):
        there = (1 - g if dg else g) * NX + (x + dx) % NX
        back = ((NX - dx) % NX) * 2 + dg
        copy = remote(
            ps_buf.at[dg, there],
            pr_buf.at[back],
            pick_send.at[back],
            pick_recv.at[back],
            at_xyg(dx, 0, dg, -4 if dg else 4),
        )
        copy.start()
        picks.append(copy)

    rows_b = []
    lane_b = lax.broadcasted_iota(jnp.int32, (64, 128), 1) & 3
    position = tp * 64 + lax.broadcasted_iota(jnp.int32, (64, 128), 0)
    for b in range(BR):
        live = jnp.logical_and(position < len_ref[0, b], lane_b == b)
        rows_b.append(jnp.where(live, 1.0, 0.0))
    mask_buf[...] = jnp.concatenate(rows_b, axis=0)
    inverse = 1.0 / math.sqrt(HD)
    loads[4].wait()
    for s in range(STEPS):
        q_ref[4 * s : 4 * s + 4] = q4_buf[s].astype(F32)

    def head_queries(kv):
        return jnp.concatenate(
            [q_ref[:, pl.ds(pl.multiple_of(kv * 1024 + h * 128, 128), 128)] for h in range(8)], axis=0
        ).astype(BF16)

    def attend(kv, carry):
        columns = pl.ds(pl.multiple_of(kv * 128, 128), 128)
        scores = (
            lax.dot_general(
                k_ref[:, columns], head_queries(kv), (((1,), (1,)), ((), ())), preferred_element_type=F32
            )
            * inverse
        )
        live = mask_buf[...] > 0.5
        masked = jnp.where(live, scores, masked_score)
        peak = jnp.max(masked, axis=0, keepdims=True)
        weights = jnp.where(live, jnp.exp(masked - peak), 0.0)
        total = jnp.sum(weights, axis=0, keepdims=True)
        part = lax.dot_general(
            v_ref[:, columns],
            weights.astype(BF16),
            (((0,), (0,)), ((), ())),
            preferred_element_type=F32,
        )
        ya_buf[kv] = part.astype(BF16)
        ys_buf[kv] = jnp.concatenate([peak, total], axis=0)
        return carry

    loads[5].wait()
    loads[6].wait()
    lax.fori_loop(0, KV // 2, attend, 0)
    pl.semaphore_wait(hello.at[0], 1)
    pl.semaphore_wait(hello.at[1], 1)
    signal(hello.at[2], at_z(8))
    signal(hello.at[3], at_z(-8))
    lax.fori_loop(KV // 2, KV, attend, 0)
    y_att = []
    for i, d in enumerate((1, 3, 2)):
        pair = pl.ds(((y + d) % NY) * 2, 2)
        y_att.append(
            (
                remote(ys_buf.at[pair], ysr_buf.at[i], y_send.at[0, i], y_recv.at[0, i], at_y(d)),
                remote(ya_buf.at[pair], yar_buf.at[i], y_send.at[1, i], y_recv.at[1, i], at_y(d)),
            )
        )
        for copy in y_att[-1]:
            copy.start()
    for copy in picks:
        copy.wait_recv()
    lhs = pr_buf[...].reshape(128, 128).astype(F32)
    upper = (lax.broadcasted_iota(jnp.int32, (128, 128), 1) & 8) == 0
    lhs = jnp.concatenate([jnp.where(upper, lhs, 0.0), jnp.where(upper, 0.0, lhs)], axis=0).astype(BF16)
    for copy in windows:
        copy.wait_recv()
    rows = w_buf[...]
    product = jnp.dot(lhs, rows.reshape(128, 512), preferred_element_type=F32).astype(BF16)
    top = jnp.max(jnp.abs(rows.astype(F32)), axis=0)
    for h in range(2):
        high = jnp.max(top[h * 8 : h * 8 + 8], axis=0, keepdims=True)
        for k in range(2):
            pm_buf[2 * h + k] = high[:, k * 256 : (k + 1) * 256]
            for i in range(8):
                first = h * 128 + i * 16
                pd_buf[i, 2 * h + k] = product[first : first + 16, k * 256 : (k + 1) * 256]
    direct = []
    for dx, dy, dg in NEAR:
        there = (y + dy) % NY
        back = (((NX - dx) % NX) * NY + (NY - dy) % NY) * 2 + dg
        peer = at_xyg(dx, dy, dg)
        direct += [
            remote(pd_buf.at[dx * 2 + dg, there], pdr_buf.at[back], d_send.at[back], d_recv.at[back], peer),
            remote(pm_buf.at[there], pmr_buf.at[back], m_send.at[back], m_recv.at[back], peer),
        ]
        direct[-2].start()
        direct[-1].start()

    for copies in y_att:
        for copy in copies:
            copy.wait_recv()
    for pair in range(2):
        stats = [ys_buf[y * 2 + pair]] + [ysr_buf[i, pair] for i in range(3)]
        parts = [ya_buf[y * 2 + pair]] + [yar_buf[i, pair] for i in range(3)]
        peak = functools.reduce(jnp.maximum, [s[0:1] for s in stats])
        factors = [jnp.exp(s[0:1] - peak) for s in stats]
        total = sum(s[1:2] * f for s, f in zip(stats, factors))
        part = sum(p.astype(F32) * f for p, f in zip(parts, factors))
        zs_buf[pair] = jnp.concatenate([peak, total], axis=0)
        turned = part.T.astype(BF16)
        za_buf[2 * pair] = turned[:64]
        za_buf[2 * pair + 1] = turned[64:]
    pl.semaphore_wait(hello.at[2], 1)
    pl.semaphore_wait(hello.at[3], 1)
    z_att = []
    for i, d in enumerate((2, 1, 3)):
        dest = (zh + d) % ZHI
        z_att.append(
            (
                remote(zs_buf.at[dest // 2], zsr_buf.at[i], z_send.at[0, i], z_recv.at[0, i], at_z(8 * d)),
                remote(za_buf.at[dest], zar_buf.at[i], z_send.at[1, i], z_recv.at[1, i], at_z(8 * d)),
            )
        )
        for copy in z_att[-1]:
            copy.start()

    for copy in direct:
        copy.wait_recv()
    added = pd_buf[0, y].astype(F32) + sum(pdr_buf[i].astype(F32) for i in range(1, 32))
    highest = functools.reduce(jnp.maximum, [pm_buf[y]] + [pmr_buf[i] for i in range(1, 32)])
    for k in range(2):
        zf_buf[k] = added[:, k * 128 : (k + 1) * 128].astype(BF16)
        zm_buf[k] = highest[:, k * 128 : (k + 1) * 128]
    z_new = []
    for i, d in enumerate((12, -12, 4, -4)):
        half = ((z + d + NZ) % NZ) // 16
        z_new.append(
            (
                remote(zf_buf.at[half], zfr_buf.at[i], n_send.at[0, i], n_recv.at[0, i], at_z(d)),
                remote(zm_buf.at[half], zmr_buf.at[i], n_send.at[1, i], n_recv.at[1, i], at_z(d)),
            )
        )
        for copy in z_new[-1]:
            copy.start()

    head = y * 2 + zh // 2
    loads[8].wait()
    own_keys = jnp.concatenate(
        [nk4_buf[s, :, pl.ds(pl.multiple_of(head * 128, 128), 128)].astype(F32) for s in range(STEPS)], axis=0
    ).astype(BF16)
    new_scores = (
        lax.dot_general(own_keys, head_queries(head), (((1,), (1,)), ((), ())), preferred_element_type=F32)
        * inverse
    )
    r = lax.broadcasted_iota(jnp.int32, (16, 128), 0)
    c = lax.broadcasted_iota(jnp.int32, (16, 128), 1)
    causal = jnp.logical_and((r & 3) == (c & 3), (r >> 2) <= ((c >> 2) & 3))
    new_scores = jnp.where(causal, new_scores, masked_score)
    new_peak = jnp.max(new_scores, axis=0, keepdims=True)

    for copies in z_att:
        for copy in copies:
            copy.wait_recv()
    stats = [zs_buf[zh // 2]] + [zsr_buf[i] for i in range(3)]
    parts = [za_buf[zh]] + [zar_buf[i] for i in range(3)]
    peak = functools.reduce(jnp.maximum, [s[0:1] for s in stats] + [new_peak])
    factors = [jnp.exp(s[0:1] - peak) for s in stats]
    new_weights = jnp.where(causal, jnp.exp(new_scores - peak), 0.0)
    denominator = sum(s[1:2] * f for s, f in zip(stats, factors)) + jnp.sum(
        new_weights, axis=0, keepdims=True
    )
    share = 1.0 / denominator
    columns = jnp.concatenate([f * share for f in factors] + [share] * 4, axis=0).T
    odd = (zh % 2) == 1
    columns = jnp.where(odd, columns[64:], columns[:64])
    merged = sum(p.astype(F32) * columns[:, i : i + 1] for i, p in enumerate(parts))

    for copies in z_new:
        for copy in copies:
            copy.wait_recv()
    values = sum(zfr_buf[i].astype(F32) for i in range(4)).astype(BF16)
    highest = functools.reduce(jnp.maximum, [zmr_buf[i] for i in range(4)])
    scales = (highest + scale_floor) / code_range
    scale_ref[...] = jnp.broadcast_to(jnp.where(odd, scales[:, 64:], scales[:, :64]), (8, 64))
    wide = values.astype(F32)
    fresh_ref[...] = jnp.where(odd, wide[:, 64:], wide[:, :64])
    mixed = lax.dot_general(
        new_weights.astype(BF16), values, (((0,), (0,)), ((), ())), preferred_element_type=F32
    )
    mixed = jnp.where(odd, mixed[64:], mixed[:64])
    result = merged + mixed * columns[:, 4:5]
    for h in range(4):
        att_ref[:, h * 128 : (h + 1) * 128] = result[h * 16 : (h + 1) * 16]

    for copy in windows + picks + direct:
        copy.wait_send()
    for copies in y_att + z_att + z_new:
        for copy in copies:
            copy.wait_send()


def finish(mw, grad, m1, m2, step, scale, fresh, att, nw_out, scale_out, fresh_out, att_out):
    nw_out[...] = adamw(mw[...], grad[...], m1[...], m2[...], step[0])
    scale_out[...] = scale[0:1]
    for s in range(STEPS):
        fresh_out[s] = fresh[4 * s : 4 * s + 4].astype(BF16)
        att_out[s] = att[4 * s : 4 * s + 4]


def body(
    master_weight,
    grad,
    moment1,
    moment2,
    step_count,
    x_new,
    queries,
    new_keys,
    cache_keys,
    cache_values,
    lengths,
):
    vmem = pl.BlockSpec(memory_space=pltpu.VMEM)
    smem = pl.BlockSpec(memory_space=pltpu.SMEM)
    hbm = pl.BlockSpec(memory_space=pl.ANY)
    dma = pltpu.SemaphoreType.DMA
    optimizer = (master_weight, grad, moment1, moment2, step_count)
    scale, fresh, attention = pl.pallas_call(
        kernel,
        out_shape=(
            jax.ShapeDtypeStruct((8, 64), F32),
            jax.ShapeDtypeStruct((16, 64), F32),
            jax.ShapeDtypeStruct((16, 512), F32),
        ),
        in_specs=[hbm] * 4 + [smem] + [hbm] * 5 + [smem],
        out_specs=(vmem,) * 3,
        scratch_shapes=[
            pltpu.VMEM((4, 8, 1024), F32),
            pltpu.VMEM((STEPS, BR, 8192), BF16),
            pltpu.VMEM((STEPS, BR, 8192), BF16),
            pltpu.VMEM((STEPS, BR, 1024), BF16),
            pltpu.VMEM((256, 1024), BF16),
            pltpu.VMEM((256, 1024), BF16),
            pltpu.VMEM((128, 1024), F32),
            pltpu.VMEM((16, 8192), F32),
            pltpu.VMEM((ZLO, 16, 512), BF16),
            pltpu.VMEM((1024, 256), BF16),
            pltpu.VMEM((2, 8, 16, 128), BF16),
            pltpu.VMEM((8, 16, 128), BF16),
            pltpu.VMEM((256, 128), F32),
            pltpu.VMEM((KV, 128, 128), BF16),
            pltpu.VMEM((KV, 2, 128), F32),
            pltpu.VMEM((3, 2, 128, 128), BF16),
            pltpu.VMEM((3, 2, 2, 128), F32),
            pltpu.VMEM((4, 64, 128), BF16),
            pltpu.VMEM((2, 2, 128), F32),
            pltpu.VMEM((3, 64, 128), BF16),
            pltpu.VMEM((3, 2, 128), F32),
            pltpu.VMEM((8, NY, 16, 256), BF16),
            pltpu.VMEM((32, 16, 256), BF16),
            pltpu.VMEM((NY, 1, 256), F32),
            pltpu.VMEM((32, 1, 256), F32),
            pltpu.VMEM((2, 16, 128), BF16),
            pltpu.VMEM((4, 16, 128), BF16),
            pltpu.VMEM((2, 1, 128), F32),
            pltpu.VMEM((4, 1, 128), F32),
            dma((9,)),
            dma((8,)),
            dma((8,)),
            dma((8,)),
            dma((8,)),
            dma((32,)),
            dma((32,)),
            dma((32,)),
            dma((32,)),
            dma((3, 3)),
            dma((3, 3)),
            dma((2, 3)),
            dma((2, 3)),
            dma((2, 4)),
            dma((2, 4)),
            pltpu.SemaphoreType.REGULAR((4,)),
        ],
        compiler_params=pltpu.CompilerParams(collective_id=0, has_side_effects=True),
    )(
        *optimizer,
        x_new,
        queries,
        new_keys,
        cache_keys.reshape(256, 1024),
        cache_values.reshape(256, 1024),
        lengths,
    )
    new_weight, scale, fresh, attention = pl.pallas_call(
        finish,
        out_shape=(
            jax.ShapeDtypeStruct((8, 1024), F32),
            jax.ShapeDtypeStruct((1, 64), F32),
            jax.ShapeDtypeStruct((STEPS, BR, 64), BF16),
            jax.ShapeDtypeStruct((STEPS, BR, 512), F32),
        ),
        in_specs=[vmem] * 4 + [smem] + [vmem] * 3,
        out_specs=(vmem,) * 4,
    )(*optimizer, scale, fresh, attention)
    return new_weight, scale[0], fresh, attention


def solution(mesh):
    return jax.shard_map(
        body,
        mesh=mesh,
        in_specs=(
            P(("group", "rep", "tp"), None),
            P(("group", "rep", "tp"), None),
            P(("group", "rep", "tp"), None),
            P(("group", "rep", "tp"), None),
            P(),
            P(None, ("group", "rep"), None),
            P(None, ("group", "rep"), None),
            P(None, ("group", "rep"), None),
            P(("group", "rep"), "tp", None),
            P(("group", "rep"), "tp", None),
            P(("group", "rep"), None),
        ),
        out_specs=(
            P(("group", "rep", "tp"), None),
            P("tp"),
            P(None, ("group", "rep"), "tp"),
            P(None, ("group", "rep"), "tp"),
        ),
        check_vma=False,
    )
```

```python
import functools
import math

import jax
import jax.numpy as jnp
from jax import lax
from jax.experimental import pallas as pl
from jax.experimental.pallas import tpu as pltpu
from jax.sharding import PartitionSpec as P

H = 64
KV = 8
HD = 128
STEPS = 4
BR = 4

beta_first = 0.9
beta_second = 0.999
learn_rate = 0.01
decay_rate = 0.1
adam_floor = 1e-08
scale_floor = 1e-06
code_range = 448.0
masked_score = -1e30

F32 = jnp.float32
BF16 = jnp.bfloat16
MESH = pl.DeviceIdType.MESH

NX, NY, ZLO, ZHI = 4, 4, 8, 4
NZ = ZLO * ZHI
SOURCES = (-4, 3, -3, 2, -2, 1, -1)
NEAR = tuple(
    (dx, dy, dg)
    for far in (4, 3, 2, 1, 0)
    for dx in range(NX)
    for dy in range(NY)
    for dg in range(2)
    if min(dx, NX - dx) + min(dy, NY - dy) == far and (dx, dy, dg) != (0, 0, 0)
)


def adamw(mw, grad, m1, m2, step):
    steps_done = jnp.full(mw.shape, step, jnp.int32).astype(F32)
    first = beta_first * m1 + (1.0 - beta_first) * grad
    second = beta_second * m2 + (1.0 - beta_second) * grad * grad
    correction = jnp.sqrt(1.0 - jnp.exp(steps_done * math.log(beta_second))) / (
        1.0 - jnp.exp(steps_done * math.log(beta_first))
    )
    return mw - learn_rate * correction * first / (jnp.sqrt(second) + adam_floor) - learn_rate * decay_rate * mw


def kernel(
    mw_hbm,
    grad_hbm,
    m1_hbm,
    m2_hbm,
    step_ref,
    x_hbm,
    q_hbm,
    nk_hbm,
    k_hbm,
    v_hbm,
    len_ref,
    scale_ref,
    fresh_ref,
    att_ref,
    rows_buf,
    x4_buf,
    q4_buf,
    nk4_buf,
    k_ref,
    v_ref,
    xf_buf,
    q_ref,
    w_buf,
    sel_mat,
    ps_buf,
    pr_buf,
    mask_buf,
    ya_buf,
    ys_buf,
    yar_buf,
    ysr_buf,
    za_buf,
    zs_buf,
    zar_buf,
    zsr_buf,
    pd_buf,
    pdr_buf,
    pm_buf,
    pmr_buf,
    zf_buf,
    zfr_buf,
    zm_buf,
    zmr_buf,
    in_sem,
    win_send,
    win_recv,
    pick_send,
    pick_recv,
    d_send,
    d_recv,
    m_send,
    m_recv,
    y_send,
    y_recv,
    z_send,
    z_recv,
    n_send,
    n_recv,
    hello,
):
    g = lax.axis_index("group")
    rep = lax.axis_index("rep")
    tp = lax.axis_index("tp")
    x, zl = rep >> 3, rep & 7
    y, zh = tp >> 2, tp & 3
    z = zh * ZLO + zl
    cores = (g, 1 - g)
    xs = [(x + d) & 3 for d in range(NX)]
    ys = [(y + d) & 3 for d in range(NY)]
    plane_rep = [v * ZLO + zl for v in xs]
    plane_tp = [v * ZHI + zh for v in ys]
    zs = {d: (z + d) & 31 for d in (1, 2, 3, 4, 8, 12, 16, 24, -1, -2, -3, -4, -8, -12)}
    z_rep = {d: x * ZLO + (v & 7) for d, v in zs.items()}
    z_tp = {d: y * ZHI + (v >> 3) for d, v in zs.items()}

    def at_z(offset):
        return (g, z_rep[offset], z_tp[offset])

    def at_y(offset):
        return (g, rep, plane_tp[offset])

    def at_xyg(dx, dy, dg):
        return (cores[dg], plane_rep[dx], plane_tp[dy])

    def at_xzg(dx, dz, dg):
        return (cores[dg], xs[dx] * ZLO + (zs[dz] & 7), z_tp[dz])

    def signal(sem, peer):
        pl.semaphore_signal(sem, inc=1, device_id=peer, device_id_type=MESH)

    def remote(src, dst, send, recv, peer):
        return pltpu.make_async_remote_copy(
            src_ref=src, dst_ref=dst, send_sem=send, recv_sem=recv, device_id=peer, device_id_type=MESH
        )

    barrier = pltpu.get_barrier_semaphore()
    peers = [at_z(d) for d in (4, -4, 3, -3, 2, -2, 1, -1)]
    peers += [at_xyg(*there) for there in NEAR]
    for peer in peers:
        signal(barrier, peer)

    loads = [
        pltpu.make_async_copy(src, dst, in_sem.at[i])
        for i, (src, dst) in enumerate(
            [(ref, rows_buf.at[i]) for i, ref in enumerate((mw_hbm, grad_hbm, m1_hbm, m2_hbm))]
            + [(q_hbm, q4_buf), (k_hbm, k_ref), (v_hbm, v_ref), (x_hbm, x4_buf), (nk_hbm, nk4_buf)]
        )
    ]
    for copy in loads:
        copy.start()

    for low in range(ZLO):
        r = lax.broadcasted_iota(jnp.int32, (128, 128), 0)
        k = lax.broadcasted_iota(jnp.int32, (128, 128), 1)
        for way in range(2):
            base = z + (0 if way == 0 else NZ - 8)
            there = (base + ((low - base + 2 * NZ) & 7)) & 31
            lanes = (y * ZHI + (there >> 3)) * 8
            hit = jnp.logical_and((k >> 4) == low, r == lanes + (k & 7))
            sel_mat[low * 128 : (low + 1) * 128, way * 128 : (way + 1) * 128] = jnp.where(
                hit, 1.0, 0.0
            ).astype(BF16)

    for copy in loads[:4]:
        copy.wait()
    nw = adamw(rows_buf[0], rows_buf[1], rows_buf[2], rows_buf[3], step_ref[0])
    w_buf[zl] = jnp.concatenate([nw[:, :512], nw[:, 512:]], axis=0).astype(BF16)

    loads[7].wait()
    for j in range(8):
        for step in range(STEPS):
            xf_buf[j * 16 + 4 * step : j * 16 + 4 * step + 4] = x4_buf[
                step, :, j * 1024 : (j + 1) * 1024
            ].astype(F32)
    picked = jnp.dot(xf_buf[...].astype(BF16), sel_mat[...], preferred_element_type=F32).astype(BF16)
    for j in range(8):
        for way in range(2):
            ps_buf[way, j] = picked[j * 16 : (j + 1) * 16, way * 128 : (way + 1) * 128]

    pl.semaphore_wait(barrier, len(peers))

    signal(hello.at[0], at_z(4))
    signal(hello.at[1], at_z(-4))
    for dx in range(NX):
        for dg in range(2):
            if dx or dg:
                signal(hello.at[4], at_xyg(dx, 0, dg))
    windows = []
    for i, e in enumerate(SOURCES):
        own = w_buf.at[zl]
        copy = remote(own, own, win_send.at[i], win_recv.at[i], at_z(-e))
        copy.start()
        windows.append(copy)
    rows_b = []
    lane_b = lax.broadcasted_iota(jnp.int32, (64, 128), 1) & 3
    position = tp * 64 + lax.broadcasted_iota(jnp.int32, (64, 128), 0)
    for b in range(BR):
        live = jnp.logical_and(position < len_ref[0, b], lane_b == b)
        rows_b.append(jnp.where(live, 1.0, 0.0))
    mask_buf[...] = jnp.concatenate(rows_b, axis=0)
    inverse = 1.0 / math.sqrt(HD)
    loads[4].wait()
    for s in range(STEPS):
        q_ref[4 * s : 4 * s + 4] = q4_buf[s].astype(F32)

    pl.semaphore_wait(hello.at[4], 7)
    picks = []
    for dx, dg in ((2, 0), (2, 1), (1, 0), (1, 1), (3, 0), (3, 1), (0, 0), (0, 1)):
        there = cores[dg] * NX + xs[dx]
        back = ((NX - dx) % NX) * 2 + dg
        copy = remote(
            ps_buf.at[dg, there],
            pr_buf.at[back],
            pick_send.at[back],
            pick_recv.at[back],
            at_xzg(dx, -4 if dg else 4, dg),
        )
        copy.start()
        picks.append(copy)

    def head_queries(kv):
        return jnp.concatenate(
            [q_ref[:, pl.ds(pl.multiple_of(kv * 1024 + h * 128, 128), 128)] for h in range(8)], axis=0
        ).astype(BF16)

    def attend(kv, carry):
        columns = pl.ds(pl.multiple_of(kv * 128, 128), 128)
        scores = (
            lax.dot_general(
                k_ref[:, columns], head_queries(kv), (((1,), (1,)), ((), ())), preferred_element_type=F32
            )
            * inverse
        )
        live = mask_buf[...] > 0.5
        masked = jnp.where(live, scores, masked_score)
        peak = jnp.max(masked, axis=0, keepdims=True)
        weights = jnp.where(live, jnp.exp(masked - peak), 0.0)
        total = jnp.sum(weights, axis=0, keepdims=True)
        part = lax.dot_general(
            v_ref[:, columns],
            weights.astype(BF16),
            (((0,), (0,)), ((), ())),
            preferred_element_type=F32,
        )
        ya_buf[kv] = part.astype(BF16)
        ys_buf[kv] = jnp.concatenate([peak, total], axis=0)
        return carry

    loads[5].wait()
    loads[6].wait()
    lax.fori_loop(0, KV // 2, attend, 0)
    pl.semaphore_wait(hello.at[0], 1)
    pl.semaphore_wait(hello.at[1], 1)
    signal(hello.at[2], at_z(8))
    signal(hello.at[3], at_z(-8))
    lax.fori_loop(KV // 2, KV, attend, 0)
    y_att = []
    for i, d in enumerate((1, 3, 2)):
        pair = pl.ds(ys[d] * 2, 2)
        y_att.append(
            (
                remote(ys_buf.at[pair], ysr_buf.at[i], y_send.at[0, i], y_recv.at[0, i], at_y(d)),
                remote(ya_buf.at[pair], yar_buf.at[i], y_send.at[1, i], y_recv.at[1, i], at_y(d)),
            )
        )
        for copy in y_att[-1]:
            copy.start()
    for copy in picks:
        copy.wait_recv()
    lhs = pr_buf[...].reshape(128, 128).astype(F32)
    upper = (lax.broadcasted_iota(jnp.int32, (128, 128), 1) & 8) == 0
    lhs = jnp.concatenate([jnp.where(upper, lhs, 0.0), jnp.where(upper, 0.0, lhs)], axis=0).astype(BF16)
    for copy in windows:
        copy.wait_recv()
    rows = w_buf[...]
    product = jnp.dot(lhs, rows.reshape(128, 512), preferred_element_type=F32).astype(BF16)
    for i in range(8):
        for h in range(2):
            for k in range(2):
                first = h * 128 + i * 16
                pd_buf[i, 2 * h + k] = product[first : first + 16, k * 256 : (k + 1) * 256]
    backs = [(((NX - dx) % NX) * NY + (NY - dy) % NY) * 2 + dg for dx, dy, dg in NEAR]
    direct = []
    for (dx, dy, dg), back in zip(NEAR, backs):
        source = pd_buf.at[dx * 2 + dg, ys[dy]]
        copy = remote(source, pdr_buf.at[back], d_send.at[back], d_recv.at[back], at_xyg(dx, dy, dg))
        copy.start()
        direct.append(copy)
    top = jnp.max(jnp.abs(rows.astype(F32)), axis=0)
    for h in range(2):
        high = jnp.max(top[h * 8 : h * 8 + 8], axis=0, keepdims=True)
        for k in range(2):
            pm_buf[2 * h + k] = high[:, k * 256 : (k + 1) * 256]
    for (dx, dy, dg), back in zip(NEAR, backs):
        copy = remote(
            pm_buf.at[ys[dy]], pmr_buf.at[back], m_send.at[back], m_recv.at[back], at_xyg(dx, dy, dg)
        )
        copy.start()
        direct.append(copy)

    for copies in y_att:
        for copy in copies:
            copy.wait_recv()
    for pair in range(2):
        stats = [ys_buf[y * 2 + pair]] + [ysr_buf[i, pair] for i in range(3)]
        parts = [ya_buf[y * 2 + pair]] + [yar_buf[i, pair] for i in range(3)]
        peak = functools.reduce(jnp.maximum, [s[0:1] for s in stats])
        factors = [jnp.exp(s[0:1] - peak) for s in stats]
        total = sum(s[1:2] * f for s, f in zip(stats, factors))
        part = sum(p.astype(F32) * f for p, f in zip(parts, factors))
        zs_buf[pair] = jnp.concatenate([peak, total], axis=0)
        turned = part.T.astype(BF16)
        za_buf[2 * pair] = turned[:64]
        za_buf[2 * pair + 1] = turned[64:]
    pl.semaphore_wait(hello.at[2], 1)
    pl.semaphore_wait(hello.at[3], 1)
    z_att = []
    for i, d in enumerate((2, 1, 3)):
        dest = (zh + d) & 3
        z_att.append(
            (
                remote(zs_buf.at[dest >> 1], zsr_buf.at[i], z_send.at[0, i], z_recv.at[0, i], at_z(8 * d)),
                remote(za_buf.at[dest], zar_buf.at[i], z_send.at[1, i], z_recv.at[1, i], at_z(8 * d)),
            )
        )
        for copy in z_att[-1]:
            copy.start()

    for copy in direct:
        copy.wait_recv()
    added = pd_buf[0, y].astype(F32) + sum(pdr_buf[i].astype(F32) for i in range(1, 32))
    highest = functools.reduce(jnp.maximum, [pm_buf[y]] + [pmr_buf[i] for i in range(1, 32)])
    for k in range(2):
        zf_buf[k] = added[:, k * 128 : (k + 1) * 128].astype(BF16)
        zm_buf[k] = highest[:, k * 128 : (k + 1) * 128]
    z_new = []
    for i, d in enumerate((12, -12, 4, -4)):
        half = zs[d] >> 4
        z_new.append(
            (
                remote(zf_buf.at[half], zfr_buf.at[i], n_send.at[0, i], n_recv.at[0, i], at_z(d)),
                remote(zm_buf.at[half], zmr_buf.at[i], n_send.at[1, i], n_recv.at[1, i], at_z(d)),
            )
        )
        for copy in z_new[-1]:
            copy.start()

    head = y * 2 + (zh >> 1)
    loads[8].wait()
    own_keys = jnp.concatenate(
        [nk4_buf[s, :, pl.ds(pl.multiple_of(head * 128, 128), 128)].astype(F32) for s in range(STEPS)], axis=0
    ).astype(BF16)
    new_scores = (
        lax.dot_general(own_keys, head_queries(head), (((1,), (1,)), ((), ())), preferred_element_type=F32)
        * inverse
    )
    r = lax.broadcasted_iota(jnp.int32, (16, 128), 0)
    c = lax.broadcasted_iota(jnp.int32, (16, 128), 1)
    causal = jnp.logical_and((r & 3) == (c & 3), (r >> 2) <= ((c >> 2) & 3))
    new_scores = jnp.where(causal, new_scores, masked_score)
    new_peak = jnp.max(new_scores, axis=0, keepdims=True)

    for copies in z_att:
        for copy in copies:
            copy.wait_recv()
    stats = [zs_buf[zh >> 1]] + [zsr_buf[i] for i in range(3)]
    parts = [za_buf[zh]] + [zar_buf[i] for i in range(3)]
    peak = functools.reduce(jnp.maximum, [s[0:1] for s in stats] + [new_peak])
    factors = [jnp.exp(s[0:1] - peak) for s in stats]
    new_weights = jnp.where(causal, jnp.exp(new_scores - peak), 0.0)
    denominator = sum(s[1:2] * f for s, f in zip(stats, factors)) + jnp.sum(
        new_weights, axis=0, keepdims=True
    )
    share = 1.0 / denominator
    columns = jnp.concatenate([f * share for f in factors] + [share] * 4, axis=0).T
    odd = (zh & 1) == 1
    columns = jnp.where(odd, columns[64:], columns[:64])
    merged = sum(p.astype(F32) * columns[:, i : i + 1] for i, p in enumerate(parts))

    for copies in z_new:
        for copy in copies:
            copy.wait_recv()
    values = sum(zfr_buf[i].astype(F32) for i in range(4)).astype(BF16)
    highest = functools.reduce(jnp.maximum, [zmr_buf[i] for i in range(4)])
    scales = (highest + scale_floor) / code_range
    scale_ref[...] = jnp.broadcast_to(jnp.where(odd, scales[:, 64:], scales[:, :64]), (8, 64))
    wide = values.astype(F32)
    fresh_ref[...] = jnp.where(odd, wide[:, 64:], wide[:, :64])
    mixed = lax.dot_general(
        new_weights.astype(BF16), values, (((0,), (0,)), ((), ())), preferred_element_type=F32
    )
    mixed = jnp.where(odd, mixed[64:], mixed[:64])
    result = merged + mixed * columns[:, 4:5]
    for h in range(4):
        att_ref[:, h * 128 : (h + 1) * 128] = result[h * 16 : (h + 1) * 16]

    for copy in windows + picks + direct:
        copy.wait_send()
    for copies in y_att + z_att + z_new:
        for copy in copies:
            copy.wait_send()


def finish(mw, grad, m1, m2, step, scale, fresh, att, nw_out, scale_out, fresh_out, att_out):
    nw_out[...] = adamw(mw[...], grad[...], m1[...], m2[...], step[0])
    scale_out[...] = scale[0:1]
    for s in range(STEPS):
        fresh_out[s] = fresh[4 * s : 4 * s + 4].astype(BF16)
        att_out[s] = att[4 * s : 4 * s + 4]


def body(
    master_weight,
    grad,
    moment1,
    moment2,
    step_count,
    x_new,
    queries,
    new_keys,
    cache_keys,
    cache_values,
    lengths,
):
    vmem = pl.BlockSpec(memory_space=pltpu.VMEM)
    smem = pl.BlockSpec(memory_space=pltpu.SMEM)
    hbm = pl.BlockSpec(memory_space=pl.ANY)
    dma = pltpu.SemaphoreType.DMA
    optimizer = (master_weight, grad, moment1, moment2, step_count)
    scale, fresh, attention = pl.pallas_call(
        kernel,
        out_shape=(
            jax.ShapeDtypeStruct((8, 64), F32),
            jax.ShapeDtypeStruct((16, 64), F32),
            jax.ShapeDtypeStruct((16, 512), F32),
        ),
        in_specs=[hbm] * 4 + [smem] + [hbm] * 5 + [smem],
        out_specs=(vmem,) * 3,
        scratch_shapes=[
            pltpu.VMEM((4, 8, 1024), F32),
            pltpu.VMEM((STEPS, BR, 8192), BF16),
            pltpu.VMEM((STEPS, BR, 8192), BF16),
            pltpu.VMEM((STEPS, BR, 1024), BF16),
            pltpu.VMEM((256, 1024), BF16),
            pltpu.VMEM((256, 1024), BF16),
            pltpu.VMEM((128, 1024), F32),
            pltpu.VMEM((16, 8192), F32),
            pltpu.VMEM((ZLO, 16, 512), BF16),
            pltpu.VMEM((1024, 256), BF16),
            pltpu.VMEM((2, 8, 16, 128), BF16),
            pltpu.VMEM((8, 16, 128), BF16),
            pltpu.VMEM((256, 128), F32),
            pltpu.VMEM((KV, 128, 128), BF16),
            pltpu.VMEM((KV, 2, 128), F32),
            pltpu.VMEM((3, 2, 128, 128), BF16),
            pltpu.VMEM((3, 2, 2, 128), F32),
            pltpu.VMEM((4, 64, 128), BF16),
            pltpu.VMEM((2, 2, 128), F32),
            pltpu.VMEM((3, 64, 128), BF16),
            pltpu.VMEM((3, 2, 128), F32),
            pltpu.VMEM((8, NY, 16, 256), BF16),
            pltpu.VMEM((32, 16, 256), BF16),
            pltpu.VMEM((NY, 1, 256), F32),
            pltpu.VMEM((32, 1, 256), F32),
            pltpu.VMEM((2, 16, 128), BF16),
            pltpu.VMEM((4, 16, 128), BF16),
            pltpu.VMEM((2, 1, 128), F32),
            pltpu.VMEM((4, 1, 128), F32),
            dma((9,)),
            dma((8,)),
            dma((8,)),
            dma((8,)),
            dma((8,)),
            dma((32,)),
            dma((32,)),
            dma((32,)),
            dma((32,)),
            dma((3, 3)),
            dma((3, 3)),
            dma((2, 3)),
            dma((2, 3)),
            dma((2, 4)),
            dma((2, 4)),
            pltpu.SemaphoreType.REGULAR((5,)),
        ],
        compiler_params=pltpu.CompilerParams(collective_id=0, has_side_effects=True),
    )(
        *optimizer,
        x_new,
        queries,
        new_keys,
        cache_keys.reshape(256, 1024),
        cache_values.reshape(256, 1024),
        lengths,
    )
    new_weight, scale, fresh, attention = pl.pallas_call(
        finish,
        out_shape=(
            jax.ShapeDtypeStruct((8, 1024), F32),
            jax.ShapeDtypeStruct((1, 64), F32),
            jax.ShapeDtypeStruct((STEPS, BR, 64), BF16),
            jax.ShapeDtypeStruct((STEPS, BR, 512), F32),
        ),
        in_specs=[vmem] * 4 + [smem] + [vmem] * 3,
        out_specs=(vmem,) * 4,
    )(*optimizer, scale, fresh, attention)
    return new_weight, scale[0], fresh, attention


def solution(mesh):
    return jax.shard_map(
        body,
        mesh=mesh,
        in_specs=(
            P(("group", "rep", "tp"), None),
            P(("group", "rep", "tp"), None),
            P(("group", "rep", "tp"), None),
            P(("group", "rep", "tp"), None),
            P(),
            P(None, ("group", "rep"), None),
            P(None, ("group", "rep"), None),
            P(None, ("group", "rep"), None),
            P(("group", "rep"), "tp", None),
            P(("group", "rep"), "tp", None),
            P(("group", "rep"), None),
        ),
        out_specs=(
            P(("group", "rep", "tp"), None),
            P("tp"),
            P(None, ("group", "rep"), "tp"),
            P(None, ("group", "rep"), "tp"),
        ),
        check_vma=False,
    )
```

```python
import functools
import math

import jax
import jax.numpy as jnp
from jax import lax
from jax.experimental import pallas as pl
from jax.experimental.pallas import tpu as pltpu
from jax.sharding import PartitionSpec as P

H = 64
KV = 8
HD = 128
STEPS = 4
BR = 4

beta_first = 0.9
beta_second = 0.999
learn_rate = 0.01
decay_rate = 0.1
adam_floor = 1e-08
scale_floor = 1e-06
code_range = 448.0
masked_score = -1e30

F32 = jnp.float32
BF16 = jnp.bfloat16
MESH = pl.DeviceIdType.MESH

NX, NY, ZLO, ZHI = 4, 4, 8, 4
NZ = ZLO * ZHI
SOURCES = (-4, 3, -3, 2, -2, 1, -1)
NEAR = tuple(
    (dx, dy, dg)
    for far in (4, 3, 2, 1, 0)
    for dx in range(NX)
    for dy in range(NY)
    for dg in range(2)
    if min(dx, NX - dx) + min(dy, NY - dy) == far and (dx, dy, dg) != (0, 0, 0)
)


def adamw(mw, grad, m1, m2, step):
    steps_done = jnp.broadcast_to(step.astype(F32), mw.shape)
    first = beta_first * m1 + (1.0 - beta_first) * grad
    second = beta_second * m2 + (1.0 - beta_second) * grad * grad
    correction = jnp.sqrt(1.0 - jnp.exp(steps_done * math.log(beta_second))) / (
        1.0 - jnp.exp(steps_done * math.log(beta_first))
    )
    return mw - learn_rate * correction * first / (jnp.sqrt(second) + adam_floor) - learn_rate * decay_rate * mw


def kernel(
    mw_hbm,
    grad_hbm,
    m1_hbm,
    m2_hbm,
    step_hbm,
    x_hbm,
    q_hbm,
    nk_hbm,
    k_hbm,
    v_hbm,
    len_hbm,
    scale_ref,
    fresh_ref,
    att_ref,
    step_ref,
    len_ref,
    rows_buf,
    x4_buf,
    q4_buf,
    nk4_buf,
    k_ref,
    v_ref,
    xf_buf,
    q_ref,
    w_buf,
    sel_mat,
    ps_buf,
    pr_buf,
    mask_buf,
    ya_buf,
    ys_buf,
    yar_buf,
    ysr_buf,
    za_buf,
    zs_buf,
    zar_buf,
    zsr_buf,
    pd_buf,
    pdr_buf,
    pm_buf,
    pmr_buf,
    zf_buf,
    zfr_buf,
    zm_buf,
    zmr_buf,
    in_sem,
    win_send,
    win_recv,
    pick_send,
    pick_recv,
    d_send,
    d_recv,
    m_send,
    m_recv,
    y_send,
    y_recv,
    z_send,
    z_recv,
    n_send,
    n_recv,
    hello,
):
    g = lax.axis_index("group")
    rep = lax.axis_index("rep")
    tp = lax.axis_index("tp")
    x, zl = rep >> 3, rep & 7
    y, zh = tp >> 2, tp & 3
    z = zh * ZLO + zl
    cores = (g, 1 - g)
    xs = [(x + d) & 3 for d in range(NX)]
    ys = [(y + d) & 3 for d in range(NY)]
    plane_rep = [v * ZLO + zl for v in xs]
    plane_tp = [v * ZHI + zh for v in ys]
    zs = {d: (z + d) & 31 for d in (1, 2, 3, 4, 8, 12, 16, 24, -1, -2, -3, -4, -8, -12)}
    z_rep = {d: x * ZLO + (v & 7) for d, v in zs.items()}
    z_tp = {d: y * ZHI + (v >> 3) for d, v in zs.items()}

    def at_z(offset):
        return (g, z_rep[offset], z_tp[offset])

    def at_y(offset):
        return (g, rep, plane_tp[offset])

    def at_xyg(dx, dy, dg):
        return (cores[dg], plane_rep[dx], plane_tp[dy])

    def at_xzg(dx, dz, dg):
        return (cores[dg], xs[dx] * ZLO + (zs[dz] & 7), z_tp[dz])

    def signal(sem, peer):
        pl.semaphore_signal(sem, inc=1, device_id=peer, device_id_type=MESH)

    def remote(src, dst, send, recv, peer):
        return pltpu.make_async_remote_copy(
            src_ref=src, dst_ref=dst, send_sem=send, recv_sem=recv, device_id=peer, device_id_type=MESH
        )

    barrier = pltpu.get_barrier_semaphore()
    peers = [at_z(d) for d in (4, -4, 3, -3, 2, -2, 1, -1)]
    peers += [at_xyg(*there) for there in NEAR]
    for peer in peers:
        signal(barrier, peer)

    loads = [
        pltpu.make_async_copy(src, dst, in_sem.at[i])
        for i, (src, dst) in enumerate(
            [(ref, rows_buf.at[i]) for i, ref in enumerate((mw_hbm, grad_hbm, m1_hbm, m2_hbm))]
            + [(q_hbm, q4_buf), (k_hbm, k_ref), (v_hbm, v_ref), (x_hbm, x4_buf), (nk_hbm, nk4_buf)]
            + [(step_hbm, step_ref), (len_hbm, len_ref)]
        )
    ]
    for copy in loads:
        copy.start()

    for low in range(ZLO):
        r = lax.broadcasted_iota(jnp.int32, (128, 128), 0)
        k = lax.broadcasted_iota(jnp.int32, (128, 128), 1)
        for way in range(2):
            base = z + (0 if way == 0 else NZ - 8)
            there = (base + ((low - base + 2 * NZ) & 7)) & 31
            lanes = (y * ZHI + (there >> 3)) * 8
            hit = jnp.logical_and((k >> 4) == low, r == lanes + (k & 7))
            sel_mat[low * 128 : (low + 1) * 128, way * 128 : (way + 1) * 128] = jnp.where(
                hit, 1.0, 0.0
            ).astype(BF16)

    for copy in loads[:4] + [loads[9]]:
        copy.wait()
    nw = adamw(rows_buf[0], rows_buf[1], rows_buf[2], rows_buf[3], step_ref[...])
    w_buf[zl] = jnp.concatenate([nw[:, :512], nw[:, 512:]], axis=0).astype(BF16)

    loads[7].wait()
    for j in range(8):
        for step in range(STEPS):
            xf_buf[j * 16 + 4 * step : j * 16 + 4 * step + 4] = x4_buf[
                step, :, j * 1024 : (j + 1) * 1024
            ].astype(F32)
    picked = jnp.dot(xf_buf[...].astype(BF16), sel_mat[...], preferred_element_type=F32).astype(BF16)
    for j in range(8):
        for way in range(2):
            ps_buf[way, j] = picked[j * 16 : (j + 1) * 16, way * 128 : (way + 1) * 128]

    pl.semaphore_wait(barrier, len(peers))

    signal(hello.at[0], at_z(4))
    signal(hello.at[1], at_z(-4))
    for dx in range(NX):
        for dg in range(2):
            if dx or dg:
                signal(hello.at[4], at_xyg(dx, 0, dg))
    windows = []
    for i, e in enumerate(SOURCES):
        own = w_buf.at[zl]
        copy = remote(own, own, win_send.at[i], win_recv.at[i], at_z(-e))
        copy.start()
        windows.append(copy)
    loads[10].wait()
    rows_b = []
    lane_b = lax.broadcasted_iota(jnp.int32, (64, 128), 1) & 3
    position = tp * 64 + lax.broadcasted_iota(jnp.int32, (64, 128), 0)
    for b in range(BR):
        live = jnp.logical_and(position < len_ref[0, b], lane_b == b)
        rows_b.append(jnp.where(live, 1.0, 0.0))
    mask_buf[...] = jnp.concatenate(rows_b, axis=0)
    inverse = 1.0 / math.sqrt(HD)
    loads[4].wait()
    for s in range(STEPS):
        q_ref[4 * s : 4 * s + 4] = q4_buf[s].astype(F32)

    pl.semaphore_wait(hello.at[4], 7)
    picks = []
    for dx, dg in ((2, 0), (2, 1), (1, 0), (1, 1), (3, 0), (3, 1), (0, 0), (0, 1)):
        there = cores[dg] * NX + xs[dx]
        back = ((NX - dx) % NX) * 2 + dg
        copy = remote(
            ps_buf.at[dg, there],
            pr_buf.at[back],
            pick_send.at[back],
            pick_recv.at[back],
            at_xzg(dx, -4 if dg else 4, dg),
        )
        copy.start()
        picks.append(copy)

    def head_queries(kv):
        return jnp.concatenate(
            [q_ref[:, pl.ds(pl.multiple_of(kv * 1024 + h * 128, 128), 128)] for h in range(8)], axis=0
        ).astype(BF16)

    def attend(kv, carry):
        columns = pl.ds(pl.multiple_of(kv * 128, 128), 128)
        scores = (
            lax.dot_general(
                k_ref[:, columns], head_queries(kv), (((1,), (1,)), ((), ())), preferred_element_type=F32
            )
            * inverse
        )
        live = mask_buf[...] > 0.5
        masked = jnp.where(live, scores, masked_score)
        peak = jnp.max(masked, axis=0, keepdims=True)
        weights = jnp.where(live, jnp.exp(masked - peak), 0.0)
        total = jnp.sum(weights, axis=0, keepdims=True)
        part = lax.dot_general(
            v_ref[:, columns],
            weights.astype(BF16),
            (((0,), (0,)), ((), ())),
            preferred_element_type=F32,
        )
        ya_buf[kv] = part.astype(BF16)
        ys_buf[kv] = jnp.concatenate([peak, total], axis=0)
        return carry

    loads[5].wait()
    loads[6].wait()
    lax.fori_loop(0, KV // 2, attend, 0)
    pl.semaphore_wait(hello.at[0], 1)
    pl.semaphore_wait(hello.at[1], 1)
    signal(hello.at[2], at_z(8))
    signal(hello.at[3], at_z(-8))
    lax.fori_loop(KV // 2, KV, attend, 0)
    y_att = []
    for i, d in enumerate((1, 3, 2)):
        pair = pl.ds(ys[d] * 2, 2)
        y_att.append(
            (
                remote(ys_buf.at[pair], ysr_buf.at[i], y_send.at[0, i], y_recv.at[0, i], at_y(d)),
                remote(ya_buf.at[pair], yar_buf.at[i], y_send.at[1, i], y_recv.at[1, i], at_y(d)),
            )
        )
        for copy in y_att[-1]:
            copy.start()
    for copy in picks:
        copy.wait_recv()
    lhs = pr_buf[...].reshape(128, 128).astype(F32)
    upper = (lax.broadcasted_iota(jnp.int32, (128, 128), 1) & 8) == 0
    lhs = jnp.concatenate([jnp.where(upper, lhs, 0.0), jnp.where(upper, 0.0, lhs)], axis=0).astype(BF16)
    for copy in windows:
        copy.wait_recv()
    rows = w_buf[...]
    product = jnp.dot(lhs, rows.reshape(128, 512), preferred_element_type=F32).astype(BF16)
    for i in range(8):
        for h in range(2):
            for k in range(2):
                first = h * 128 + i * 16
                pd_buf[i, 2 * h + k] = product[first : first + 16, k * 256 : (k + 1) * 256]
    backs = [(((NX - dx) % NX) * NY + (NY - dy) % NY) * 2 + dg for dx, dy, dg in NEAR]
    direct = []
    for (dx, dy, dg), back in zip(NEAR, backs):
        source = pd_buf.at[dx * 2 + dg, ys[dy]]
        copy = remote(source, pdr_buf.at[back], d_send.at[back], d_recv.at[back], at_xyg(dx, dy, dg))
        copy.start()
        direct.append(copy)
    top = jnp.max(jnp.abs(rows.astype(F32)), axis=0)
    for h in range(2):
        high = jnp.max(top[h * 8 : h * 8 + 8], axis=0, keepdims=True)
        for k in range(2):
            pm_buf[2 * h + k] = high[:, k * 256 : (k + 1) * 256]
    for (dx, dy, dg), back in zip(NEAR, backs):
        copy = remote(
            pm_buf.at[ys[dy]], pmr_buf.at[back], m_send.at[back], m_recv.at[back], at_xyg(dx, dy, dg)
        )
        copy.start()
        direct.append(copy)

    for copies in y_att:
        for copy in copies:
            copy.wait_recv()
    for pair in range(2):
        stats = [ys_buf[y * 2 + pair]] + [ysr_buf[i, pair] for i in range(3)]
        parts = [ya_buf[y * 2 + pair]] + [yar_buf[i, pair] for i in range(3)]
        peak = functools.reduce(jnp.maximum, [s[0:1] for s in stats])
        factors = [jnp.exp(s[0:1] - peak) for s in stats]
        total = sum(s[1:2] * f for s, f in zip(stats, factors))
        part = sum(p.astype(F32) * f for p, f in zip(parts, factors))
        zs_buf[pair] = jnp.concatenate([peak, total], axis=0)
        turned = part.T.astype(BF16)
        za_buf[2 * pair] = turned[:64]
        za_buf[2 * pair + 1] = turned[64:]
    pl.semaphore_wait(hello.at[2], 1)
    pl.semaphore_wait(hello.at[3], 1)
    z_att = []
    for i, d in enumerate((2, 1, 3)):
        dest = (zh + d) & 3
        z_att.append(
            (
                remote(zs_buf.at[dest >> 1], zsr_buf.at[i], z_send.at[0, i], z_recv.at[0, i], at_z(8 * d)),
                remote(za_buf.at[dest], zar_buf.at[i], z_send.at[1, i], z_recv.at[1, i], at_z(8 * d)),
            )
        )
        for copy in z_att[-1]:
            copy.start()

    for copy in direct:
        copy.wait_recv()
    added = pd_buf[0, y].astype(F32) + sum(pdr_buf[i].astype(F32) for i in range(1, 32))
    highest = functools.reduce(jnp.maximum, [pm_buf[y]] + [pmr_buf[i] for i in range(1, 32)])
    for k in range(2):
        zf_buf[k] = added[:, k * 128 : (k + 1) * 128].astype(BF16)
        zm_buf[k] = highest[:, k * 128 : (k + 1) * 128]
    z_new = []
    for i, d in enumerate((12, -12, 4, -4)):
        half = zs[d] >> 4
        z_new.append(
            (
                remote(zf_buf.at[half], zfr_buf.at[i], n_send.at[0, i], n_recv.at[0, i], at_z(d)),
                remote(zm_buf.at[half], zmr_buf.at[i], n_send.at[1, i], n_recv.at[1, i], at_z(d)),
            )
        )
        for copy in z_new[-1]:
            copy.start()

    head = y * 2 + (zh >> 1)
    loads[8].wait()
    own_keys = jnp.concatenate(
        [nk4_buf[s, :, pl.ds(pl.multiple_of(head * 128, 128), 128)].astype(F32) for s in range(STEPS)], axis=0
    ).astype(BF16)
    new_scores = (
        lax.dot_general(own_keys, head_queries(head), (((1,), (1,)), ((), ())), preferred_element_type=F32)
        * inverse
    )
    r = lax.broadcasted_iota(jnp.int32, (16, 128), 0)
    c = lax.broadcasted_iota(jnp.int32, (16, 128), 1)
    causal = jnp.logical_and((r & 3) == (c & 3), (r >> 2) <= ((c >> 2) & 3))
    new_scores = jnp.where(causal, new_scores, masked_score)
    new_peak = jnp.max(new_scores, axis=0, keepdims=True)

    for copies in z_att:
        for copy in copies:
            copy.wait_recv()
    stats = [zs_buf[zh >> 1]] + [zsr_buf[i] for i in range(3)]
    parts = [za_buf[zh]] + [zar_buf[i] for i in range(3)]
    peak = functools.reduce(jnp.maximum, [s[0:1] for s in stats] + [new_peak])
    factors = [jnp.exp(s[0:1] - peak) for s in stats]
    new_weights = jnp.where(causal, jnp.exp(new_scores - peak), 0.0)
    denominator = sum(s[1:2] * f for s, f in zip(stats, factors)) + jnp.sum(
        new_weights, axis=0, keepdims=True
    )
    share = 1.0 / denominator
    columns = jnp.concatenate([f * share for f in factors] + [share] * 4, axis=0).T
    odd = (zh & 1) == 1
    columns = jnp.where(odd, columns[64:], columns[:64])
    merged = sum(p.astype(F32) * columns[:, i : i + 1] for i, p in enumerate(parts))

    for copies in z_new:
        for copy in copies:
            copy.wait_recv()
    values = sum(zfr_buf[i].astype(F32) for i in range(4)).astype(BF16)
    highest = functools.reduce(jnp.maximum, [zmr_buf[i] for i in range(4)])
    scales = (highest + scale_floor) / code_range
    scale_ref[...] = jnp.broadcast_to(jnp.where(odd, scales[:, 64:], scales[:, :64]), (8, 64))
    wide = values.astype(F32)
    fresh_ref[...] = jnp.where(odd, wide[:, 64:], wide[:, :64])
    mixed = lax.dot_general(
        new_weights.astype(BF16), values, (((0,), (0,)), ((), ())), preferred_element_type=F32
    )
    mixed = jnp.where(odd, mixed[64:], mixed[:64])
    result = merged + mixed * columns[:, 4:5]
    for h in range(4):
        att_ref[:, h * 128 : (h + 1) * 128] = result[h * 16 : (h + 1) * 16]

    for copy in windows + picks + direct:
        copy.wait_send()
    for copies in y_att + z_att + z_new:
        for copy in copies:
            copy.wait_send()


def finish(mw, grad, m1, m2, step, scale, fresh, att, nw_out, scale_out, fresh_out, att_out):
    nw_out[...] = adamw(mw[...], grad[...], m1[...], m2[...], step[...])
    scale_out[...] = scale[0:1]
    for s in range(STEPS):
        fresh_out[s] = fresh[4 * s : 4 * s + 4].astype(BF16)
        att_out[s] = att[4 * s : 4 * s + 4]


def body(
    master_weight,
    grad,
    moment1,
    moment2,
    step_count,
    x_new,
    queries,
    new_keys,
    cache_keys,
    cache_values,
    lengths,
):
    vmem = pl.BlockSpec(memory_space=pltpu.VMEM)
    hbm = pl.BlockSpec(memory_space=pl.ANY)
    dma = pltpu.SemaphoreType.DMA
    optimizer = (master_weight, grad, moment1, moment2, step_count.reshape(1, 1))
    scale, fresh, attention = pl.pallas_call(
        kernel,
        out_shape=(
            pltpu.VMEM((8, 64), F32),
            pltpu.VMEM((16, 64), F32),
            pltpu.VMEM((16, 512), F32),
        ),
        in_specs=[hbm] * 11,
        out_specs=(vmem,) * 3,
        scratch_shapes=[
            pltpu.VMEM((1, 1), jnp.int32),
            pltpu.SMEM((1, 4), jnp.int32),
            pltpu.VMEM((4, 8, 1024), F32),
            pltpu.VMEM((STEPS, BR, 8192), BF16),
            pltpu.VMEM((STEPS, BR, 8192), BF16),
            pltpu.VMEM((STEPS, BR, 1024), BF16),
            pltpu.VMEM((256, 1024), BF16),
            pltpu.VMEM((256, 1024), BF16),
            pltpu.VMEM((128, 1024), F32),
            pltpu.VMEM((16, 8192), F32),
            pltpu.VMEM((ZLO, 16, 512), BF16),
            pltpu.VMEM((1024, 256), BF16),
            pltpu.VMEM((2, 8, 16, 128), BF16),
            pltpu.VMEM((8, 16, 128), BF16),
            pltpu.VMEM((256, 128), F32),
            pltpu.VMEM((KV, 128, 128), BF16),
            pltpu.VMEM((KV, 2, 128), F32),
            pltpu.VMEM((3, 2, 128, 128), BF16),
            pltpu.VMEM((3, 2, 2, 128), F32),
            pltpu.VMEM((4, 64, 128), BF16),
            pltpu.VMEM((2, 2, 128), F32),
            pltpu.VMEM((3, 64, 128), BF16),
            pltpu.VMEM((3, 2, 128), F32),
            pltpu.VMEM((8, NY, 16, 256), BF16),
            pltpu.VMEM((32, 16, 256), BF16),
            pltpu.VMEM((NY, 1, 256), F32),
            pltpu.VMEM((32, 1, 256), F32),
            pltpu.VMEM((2, 16, 128), BF16),
            pltpu.VMEM((4, 16, 128), BF16),
            pltpu.VMEM((2, 1, 128), F32),
            pltpu.VMEM((4, 1, 128), F32),
            dma((11,)),
            dma((8,)),
            dma((8,)),
            dma((8,)),
            dma((8,)),
            dma((32,)),
            dma((32,)),
            dma((32,)),
            dma((32,)),
            dma((3, 3)),
            dma((3, 3)),
            dma((2, 3)),
            dma((2, 3)),
            dma((2, 4)),
            dma((2, 4)),
            pltpu.SemaphoreType.REGULAR((5,)),
        ],
        compiler_params=pltpu.CompilerParams(collective_id=0, has_side_effects=True),
    )(
        *optimizer,
        x_new,
        queries,
        new_keys,
        cache_keys.reshape(256, 1024),
        cache_values.reshape(256, 1024),
        lengths,
    )
    new_weight, scale, fresh, attention = pl.pallas_call(
        finish,
        out_shape=(
            jax.ShapeDtypeStruct((8, 1024), F32),
            jax.ShapeDtypeStruct((1, 64), F32),
            jax.ShapeDtypeStruct((STEPS, BR, 64), BF16),
            jax.ShapeDtypeStruct((STEPS, BR, 512), F32),
        ),
        in_specs=[vmem] * 8,
        out_specs=(vmem,) * 4,
    )(*optimizer, *(pltpu.with_memory_space_constraint(a, pltpu.VMEM) for a in (scale, fresh, attention)))
    return new_weight, scale[0], fresh, attention


def solution(mesh):
    return jax.shard_map(
        body,
        mesh=mesh,
        in_specs=(
            P(("group", "rep", "tp"), None),
            P(("group", "rep", "tp"), None),
            P(("group", "rep", "tp"), None),
            P(("group", "rep", "tp"), None),
            P(),
            P(None, ("group", "rep"), None),
            P(None, ("group", "rep"), None),
            P(None, ("group", "rep"), None),
            P(("group", "rep"), "tp", None),
            P(("group", "rep"), "tp", None),
            P(("group", "rep"), None),
        ),
        out_specs=(
            P(("group", "rep", "tp"), None),
            P("tp"),
            P(None, ("group", "rep"), "tp"),
            P(None, ("group", "rep"), "tp"),
        ),
        check_vma=False,
    )
```

```python
import functools
import math

import jax
import jax.numpy as jnp
from jax import lax
from jax.experimental import pallas as pl
from jax.experimental.pallas import tpu as pltpu
from jax.sharding import PartitionSpec as P

H = 64
KV = 8
HD = 128
STEPS = 4
BR = 4

beta_first = 0.9
beta_second = 0.999
learn_rate = 0.01
decay_rate = 0.1
adam_floor = 1e-08
scale_floor = 1e-06
code_range = 448.0
masked_score = -1e30

F32 = jnp.float32
BF16 = jnp.bfloat16
MESH = pl.DeviceIdType.MESH

NX, NY, ZLO, ZHI = 4, 4, 8, 4
NZ = ZLO * ZHI
SOURCES = (-4, 3, -3, 2, -2, 1, -1)
NEAR = tuple(
    (dx, dy, dg)
    for far in (4, 3, 2, 1, 0)
    for dx in range(NX)
    for dy in range(NY)
    for dg in range(2)
    if min(dx, NX - dx) + min(dy, NY - dy) == far and (dx, dy, dg) != (0, 0, 0)
)


def adamw(mw, grad, m1, m2, step):
    steps_done = jnp.broadcast_to(step.astype(F32), mw.shape)
    first = beta_first * m1 + (1.0 - beta_first) * grad
    second = beta_second * m2 + (1.0 - beta_second) * grad * grad
    correction = jnp.sqrt(1.0 - jnp.exp(steps_done * math.log(beta_second))) / (
        1.0 - jnp.exp(steps_done * math.log(beta_first))
    )
    return mw - learn_rate * correction * first / (jnp.sqrt(second) + adam_floor) - learn_rate * decay_rate * mw


def kernel(
    mw_hbm,
    grad_hbm,
    m1_hbm,
    m2_hbm,
    step_hbm,
    x_hbm,
    q_hbm,
    nk_hbm,
    k_hbm,
    v_hbm,
    len_hbm,
    nw_ref,
    scale_ref,
    fresh_ref,
    att_ref,
    step_ref,
    len_ref,
    rows_buf,
    x4_buf,
    q4_buf,
    nk4_buf,
    k_ref,
    v_ref,
    xf_buf,
    q_ref,
    w_buf,
    sel_mat,
    ps_buf,
    pr_buf,
    mask_buf,
    ya_buf,
    ys_buf,
    yar_buf,
    ysr_buf,
    za_buf,
    zs_buf,
    zar_buf,
    zsr_buf,
    pd_buf,
    pdr_buf,
    pm_buf,
    pmr_buf,
    zf_buf,
    zfr_buf,
    zm_buf,
    zmr_buf,
    in_sem,
    win_send,
    win_recv,
    pick_send,
    pick_recv,
    d_send,
    d_recv,
    m_send,
    m_recv,
    y_send,
    y_recv,
    z_send,
    z_recv,
    n_send,
    n_recv,
    hello,
):
    g = lax.axis_index("group")
    rep = lax.axis_index("rep")
    tp = lax.axis_index("tp")
    x, zl = rep >> 3, rep & 7
    y, zh = tp >> 2, tp & 3
    z = zh * ZLO + zl
    cores = (g, 1 - g)
    xs = [(x + d) & 3 for d in range(NX)]
    ys = [(y + d) & 3 for d in range(NY)]
    plane_rep = [v * ZLO + zl for v in xs]
    plane_tp = [v * ZHI + zh for v in ys]
    zs = {d: (z + d) & 31 for d in (1, 2, 3, 4, 8, 12, 16, 24, -1, -2, -3, -4, -8, -12)}
    z_rep = {d: x * ZLO + (v & 7) for d, v in zs.items()}
    z_tp = {d: y * ZHI + (v >> 3) for d, v in zs.items()}

    def at_z(offset):
        return (g, z_rep[offset], z_tp[offset])

    def at_y(offset):
        return (g, rep, plane_tp[offset])

    def at_xyg(dx, dy, dg):
        return (cores[dg], plane_rep[dx], plane_tp[dy])

    def at_xzg(dx, dz, dg):
        return (cores[dg], xs[dx] * ZLO + (zs[dz] & 7), z_tp[dz])

    def signal(sem, peer):
        pl.semaphore_signal(sem, inc=1, device_id=peer, device_id_type=MESH)

    def remote(src, dst, send, recv, peer):
        return pltpu.make_async_remote_copy(
            src_ref=src, dst_ref=dst, send_sem=send, recv_sem=recv, device_id=peer, device_id_type=MESH
        )

    barrier = pltpu.get_barrier_semaphore()
    peers = [at_z(d) for d in (4, -4, 3, -3, 2, -2, 1, -1)]
    peers += [at_xyg(*there) for there in NEAR]
    for peer in peers:
        signal(barrier, peer)

    loads = [
        pltpu.make_async_copy(src, dst, in_sem.at[i])
        for i, (src, dst) in enumerate(
            [(ref, rows_buf.at[i]) for i, ref in enumerate((mw_hbm, grad_hbm, m1_hbm, m2_hbm))]
            + [(q_hbm, q4_buf), (k_hbm, k_ref), (v_hbm, v_ref), (x_hbm, x4_buf), (nk_hbm, nk4_buf)]
            + [(step_hbm, step_ref), (len_hbm, len_ref)]
        )
    ]
    for copy in loads:
        copy.start()

    for low in range(ZLO):
        r = lax.broadcasted_iota(jnp.int32, (128, 128), 0)
        k = lax.broadcasted_iota(jnp.int32, (128, 128), 1)
        for way in range(2):
            base = z + (0 if way == 0 else NZ - 8)
            there = (base + ((low - base + 2 * NZ) & 7)) & 31
            lanes = (y * ZHI + (there >> 3)) * 8
            hit = jnp.logical_and((k >> 4) == low, r == lanes + (k & 7))
            sel_mat[low * 128 : (low + 1) * 128, way * 128 : (way + 1) * 128] = jnp.where(
                hit, 1.0, 0.0
            ).astype(BF16)

    for copy in loads[:4] + [loads[9]]:
        copy.wait()
    nw = adamw(rows_buf[0], rows_buf[1], rows_buf[2], rows_buf[3], step_ref[...])
    nw_ref[...] = nw
    w_buf[zl] = jnp.concatenate([nw[:, :512], nw[:, 512:]], axis=0).astype(BF16)

    loads[7].wait()
    for j in range(8):
        for step in range(STEPS):
            xf_buf[j * 16 + 4 * step : j * 16 + 4 * step + 4] = x4_buf[
                step, :, j * 1024 : (j + 1) * 1024
            ].astype(F32)
    picked = jnp.dot(xf_buf[...].astype(BF16), sel_mat[...], preferred_element_type=F32).astype(BF16)
    for j in range(8):
        for way in range(2):
            ps_buf[way, j] = picked[j * 16 : (j + 1) * 16, way * 128 : (way + 1) * 128]

    pl.semaphore_wait(barrier, len(peers))

    signal(hello.at[0], at_z(4))
    signal(hello.at[1], at_z(-4))
    for dx in range(NX):
        for dg in range(2):
            if dx or dg:
                signal(hello.at[4], at_xyg(dx, 0, dg))
    windows = []
    for i, e in enumerate(SOURCES):
        own = w_buf.at[zl]
        copy = remote(own, own, win_send.at[i], win_recv.at[i], at_z(-e))
        copy.start()
        windows.append(copy)
    loads[10].wait()
    rows_b = []
    lane_b = lax.broadcasted_iota(jnp.int32, (64, 128), 1) & 3
    position = tp * 64 + lax.broadcasted_iota(jnp.int32, (64, 128), 0)
    for b in range(BR):
        live = jnp.logical_and(position < len_ref[0, b], lane_b == b)
        rows_b.append(jnp.where(live, 1.0, 0.0))
    mask_buf[...] = jnp.concatenate(rows_b, axis=0)
    inverse = 1.0 / math.sqrt(HD)
    loads[4].wait()
    for s in range(STEPS):
        q_ref[4 * s : 4 * s + 4] = q4_buf[s].astype(F32)

    pl.semaphore_wait(hello.at[4], 7)
    picks = []
    for dx, dg in ((2, 0), (2, 1), (1, 0), (1, 1), (3, 0), (3, 1), (0, 0), (0, 1)):
        there = cores[dg] * NX + xs[dx]
        back = ((NX - dx) % NX) * 2 + dg
        copy = remote(
            ps_buf.at[dg, there],
            pr_buf.at[back],
            pick_send.at[back],
            pick_recv.at[back],
            at_xzg(dx, -4 if dg else 4, dg),
        )
        copy.start()
        picks.append(copy)

    def head_queries(kv):
        return jnp.concatenate(
            [q_ref[:, pl.ds(pl.multiple_of(kv * 1024 + h * 128, 128), 128)] for h in range(8)], axis=0
        ).astype(BF16)

    def attend(kv, carry):
        columns = pl.ds(pl.multiple_of(kv * 128, 128), 128)
        scores = (
            lax.dot_general(
                k_ref[:, columns], head_queries(kv), (((1,), (1,)), ((), ())), preferred_element_type=F32
            )
            * inverse
        )
        live = mask_buf[...] > 0.5
        masked = jnp.where(live, scores, masked_score)
        peak = jnp.max(masked, axis=0, keepdims=True)
        weights = jnp.where(live, jnp.exp(masked - peak), 0.0)
        total = jnp.sum(weights, axis=0, keepdims=True)
        part = lax.dot_general(
            v_ref[:, columns],
            weights.astype(BF16),
            (((0,), (0,)), ((), ())),
            preferred_element_type=F32,
        )
        ya_buf[kv] = part.astype(BF16)
        ys_buf[kv] = jnp.concatenate([peak, total], axis=0)
        return carry

    loads[5].wait()
    loads[6].wait()
    lax.fori_loop(0, KV // 2, attend, 0)
    pl.semaphore_wait(hello.at[0], 1)
    pl.semaphore_wait(hello.at[1], 1)
    signal(hello.at[2], at_z(8))
    signal(hello.at[3], at_z(-8))
    lax.fori_loop(KV // 2, KV, attend, 0)
    y_att = []
    for i, d in enumerate((1, 3, 2)):
        pair = pl.ds(ys[d] * 2, 2)
        y_att.append(
            (
                remote(ys_buf.at[pair], ysr_buf.at[i], y_send.at[0, i], y_recv.at[0, i], at_y(d)),
                remote(ya_buf.at[pair], yar_buf.at[i], y_send.at[1, i], y_recv.at[1, i], at_y(d)),
            )
        )
        for copy in y_att[-1]:
            copy.start()
    for copy in picks:
        copy.wait_recv()
    lhs = pr_buf[...].reshape(128, 128).astype(F32)
    upper = (lax.broadcasted_iota(jnp.int32, (128, 128), 1) & 8) == 0
    lhs = jnp.concatenate([jnp.where(upper, lhs, 0.0), jnp.where(upper, 0.0, lhs)], axis=0).astype(BF16)
    for copy in windows:
        copy.wait_recv()
    rows = w_buf[...]
    product = jnp.dot(lhs, rows.reshape(128, 512), preferred_element_type=F32).astype(BF16)
    for i in range(8):
        for h in range(2):
            for k in range(2):
                first = h * 128 + i * 16
                pd_buf[i, 2 * h + k] = product[first : first + 16, k * 256 : (k + 1) * 256]
    backs = [(((NX - dx) % NX) * NY + (NY - dy) % NY) * 2 + dg for dx, dy, dg in NEAR]
    direct = []
    for (dx, dy, dg), back in zip(NEAR, backs):
        source = pd_buf.at[dx * 2 + dg, ys[dy]]
        copy = remote(source, pdr_buf.at[back], d_send.at[back], d_recv.at[back], at_xyg(dx, dy, dg))
        copy.start()
        direct.append(copy)
    top = jnp.max(jnp.abs(rows.astype(F32)), axis=0)
    for h in range(2):
        high = jnp.max(top[h * 8 : h * 8 + 8], axis=0, keepdims=True)
        for k in range(2):
            pm_buf[2 * h + k] = high[:, k * 256 : (k + 1) * 256]
    for (dx, dy, dg), back in zip(NEAR, backs):
        copy = remote(
            pm_buf.at[ys[dy]], pmr_buf.at[back], m_send.at[back], m_recv.at[back], at_xyg(dx, dy, dg)
        )
        copy.start()
        direct.append(copy)

    for copies in y_att:
        for copy in copies:
            copy.wait_recv()
    for pair in range(2):
        stats = [ys_buf[y * 2 + pair]] + [ysr_buf[i, pair] for i in range(3)]
        parts = [ya_buf[y * 2 + pair]] + [yar_buf[i, pair] for i in range(3)]
        peak = functools.reduce(jnp.maximum, [s[0:1] for s in stats])
        factors = [jnp.exp(s[0:1] - peak) for s in stats]
        total = sum(s[1:2] * f for s, f in zip(stats, factors))
        part = sum(p.astype(F32) * f for p, f in zip(parts, factors))
        zs_buf[pair] = jnp.concatenate([peak, total], axis=0)
        turned = part.T.astype(BF16)
        za_buf[2 * pair] = turned[:64]
        za_buf[2 * pair + 1] = turned[64:]
    pl.semaphore_wait(hello.at[2], 1)
    pl.semaphore_wait(hello.at[3], 1)
    z_att = []
    for i, d in enumerate((2, 1, 3)):
        dest = (zh + d) & 3
        z_att.append(
            (
                remote(zs_buf.at[dest >> 1], zsr_buf.at[i], z_send.at[0, i], z_recv.at[0, i], at_z(8 * d)),
                remote(za_buf.at[dest], zar_buf.at[i], z_send.at[1, i], z_recv.at[1, i], at_z(8 * d)),
            )
        )
        for copy in z_att[-1]:
            copy.start()

    for copy in direct:
        copy.wait_recv()
    added = pd_buf[0, y].astype(F32) + sum(pdr_buf[i].astype(F32) for i in range(1, 32))
    highest = functools.reduce(jnp.maximum, [pm_buf[y]] + [pmr_buf[i] for i in range(1, 32)])
    for k in range(2):
        zf_buf[k] = added[:, k * 128 : (k + 1) * 128].astype(BF16)
        zm_buf[k] = highest[:, k * 128 : (k + 1) * 128]
    z_new = []
    for i, d in enumerate((12, -12, 4, -4)):
        half = zs[d] >> 4
        z_new.append(
            (
                remote(zf_buf.at[half], zfr_buf.at[i], n_send.at[0, i], n_recv.at[0, i], at_z(d)),
                remote(zm_buf.at[half], zmr_buf.at[i], n_send.at[1, i], n_recv.at[1, i], at_z(d)),
            )
        )
        for copy in z_new[-1]:
            copy.start()

    head = y * 2 + (zh >> 1)
    loads[8].wait()
    own_keys = jnp.concatenate(
        [nk4_buf[s, :, pl.ds(pl.multiple_of(head * 128, 128), 128)].astype(F32) for s in range(STEPS)], axis=0
    ).astype(BF16)
    new_scores = (
        lax.dot_general(own_keys, head_queries(head), (((1,), (1,)), ((), ())), preferred_element_type=F32)
        * inverse
    )
    r = lax.broadcasted_iota(jnp.int32, (16, 128), 0)
    c = lax.broadcasted_iota(jnp.int32, (16, 128), 1)
    causal = jnp.logical_and((r & 3) == (c & 3), (r >> 2) <= ((c >> 2) & 3))
    new_scores = jnp.where(causal, new_scores, masked_score)
    new_peak = jnp.max(new_scores, axis=0, keepdims=True)

    for copies in z_att:
        for copy in copies:
            copy.wait_recv()
    stats = [zs_buf[zh >> 1]] + [zsr_buf[i] for i in range(3)]
    parts = [za_buf[zh]] + [zar_buf[i] for i in range(3)]
    peak = functools.reduce(jnp.maximum, [s[0:1] for s in stats] + [new_peak])
    factors = [jnp.exp(s[0:1] - peak) for s in stats]
    new_weights = jnp.where(causal, jnp.exp(new_scores - peak), 0.0)
    denominator = sum(s[1:2] * f for s, f in zip(stats, factors)) + jnp.sum(
        new_weights, axis=0, keepdims=True
    )
    share = 1.0 / denominator
    columns = jnp.concatenate([f * share for f in factors] + [share] * 4, axis=0).T
    odd = (zh & 1) == 1
    columns = jnp.where(odd, columns[64:], columns[:64])
    merged = sum(p.astype(F32) * columns[:, i : i + 1] for i, p in enumerate(parts))

    for copies in z_new:
        for copy in copies:
            copy.wait_recv()
    values = sum(zfr_buf[i].astype(F32) for i in range(4)).astype(BF16)
    highest = functools.reduce(jnp.maximum, [zmr_buf[i] for i in range(4)])
    scales = (highest + scale_floor) / code_range
    scale_ref[...] = jnp.broadcast_to(jnp.where(odd, scales[:, 64:], scales[:, :64]), (8, 64))
    wide = values.astype(F32)
    fresh_ref[...] = jnp.where(odd, wide[:, 64:], wide[:, :64])
    mixed = lax.dot_general(
        new_weights.astype(BF16), values, (((0,), (0,)), ((), ())), preferred_element_type=F32
    )
    mixed = jnp.where(odd, mixed[64:], mixed[:64])
    result = merged + mixed * columns[:, 4:5]
    for h in range(4):
        att_ref[:, h * 128 : (h + 1) * 128] = result[h * 16 : (h + 1) * 16]

    for copy in windows + picks + direct:
        copy.wait_send()
    for copies in y_att + z_att + z_new:
        for copy in copies:
            copy.wait_send()


def finish(nw, scale, fresh, att, nw_out, scale_out, fresh_out, att_out):
    nw_out[...] = nw[...]
    scale_out[...] = scale[0:1]
    for s in range(STEPS):
        fresh_out[s] = fresh[4 * s : 4 * s + 4].astype(BF16)
        att_out[s] = att[4 * s : 4 * s + 4]


def body(
    master_weight,
    grad,
    moment1,
    moment2,
    step_count,
    x_new,
    queries,
    new_keys,
    cache_keys,
    cache_values,
    lengths,
):
    vmem = pl.BlockSpec(memory_space=pltpu.VMEM)
    hbm = pl.BlockSpec(memory_space=pl.ANY)
    dma = pltpu.SemaphoreType.DMA
    optimizer = (master_weight, grad, moment1, moment2, step_count.reshape(1, 1))
    new_weight, scale, fresh, attention = pl.pallas_call(
        kernel,
        out_shape=(
            pltpu.VMEM((8, 1024), F32),
            pltpu.VMEM((8, 64), F32),
            pltpu.VMEM((16, 64), F32),
            pltpu.VMEM((16, 512), F32),
        ),
        in_specs=[hbm] * 11,
        out_specs=(vmem,) * 4,
        scratch_shapes=[
            pltpu.VMEM((1, 1), jnp.int32),
            pltpu.SMEM((1, 4), jnp.int32),
            pltpu.VMEM((4, 8, 1024), F32),
            pltpu.VMEM((STEPS, BR, 8192), BF16),
            pltpu.VMEM((STEPS, BR, 8192), BF16),
            pltpu.VMEM((STEPS, BR, 1024), BF16),
            pltpu.VMEM((256, 1024), BF16),
            pltpu.VMEM((256, 1024), BF16),
            pltpu.VMEM((128, 1024), F32),
            pltpu.VMEM((16, 8192), F32),
            pltpu.VMEM((ZLO, 16, 512), BF16),
            pltpu.VMEM((1024, 256), BF16),
            pltpu.VMEM((2, 8, 16, 128), BF16),
            pltpu.VMEM((8, 16, 128), BF16),
            pltpu.VMEM((256, 128), F32),
            pltpu.VMEM((KV, 128, 128), BF16),
            pltpu.VMEM((KV, 2, 128), F32),
            pltpu.VMEM((3, 2, 128, 128), BF16),
            pltpu.VMEM((3, 2, 2, 128), F32),
            pltpu.VMEM((4, 64, 128), BF16),
            pltpu.VMEM((2, 2, 128), F32),
            pltpu.VMEM((3, 64, 128), BF16),
            pltpu.VMEM((3, 2, 128), F32),
            pltpu.VMEM((8, NY, 16, 256), BF16),
            pltpu.VMEM((32, 16, 256), BF16),
            pltpu.VMEM((NY, 1, 256), F32),
            pltpu.VMEM((32, 1, 256), F32),
            pltpu.VMEM((2, 16, 128), BF16),
            pltpu.VMEM((4, 16, 128), BF16),
            pltpu.VMEM((2, 1, 128), F32),
            pltpu.VMEM((4, 1, 128), F32),
            dma((11,)),
            dma((8,)),
            dma((8,)),
            dma((8,)),
            dma((8,)),
            dma((32,)),
            dma((32,)),
            dma((32,)),
            dma((32,)),
            dma((3, 3)),
            dma((3, 3)),
            dma((2, 3)),
            dma((2, 3)),
            dma((2, 4)),
            dma((2, 4)),
            pltpu.SemaphoreType.REGULAR((5,)),
        ],
        compiler_params=pltpu.CompilerParams(collective_id=0, has_side_effects=True),
    )(
        *optimizer,
        x_new,
        queries,
        new_keys,
        cache_keys.reshape(256, 1024),
        cache_values.reshape(256, 1024),
        lengths,
    )
    new_weight, scale, fresh, attention = pl.pallas_call(
        finish,
        out_shape=(
            jax.ShapeDtypeStruct((8, 1024), F32),
            jax.ShapeDtypeStruct((1, 64), F32),
            jax.ShapeDtypeStruct((STEPS, BR, 64), BF16),
            jax.ShapeDtypeStruct((STEPS, BR, 512), F32),
        ),
        in_specs=[vmem] * 4,
        out_specs=(vmem,) * 4,
    )(*(pltpu.with_memory_space_constraint(a, pltpu.VMEM) for a in (new_weight, scale, fresh, attention)))
    return new_weight, scale[0], fresh, attention


def solution(mesh):
    return jax.shard_map(
        body,
        mesh=mesh,
        in_specs=(
            P(("group", "rep", "tp"), None),
            P(("group", "rep", "tp"), None),
            P(("group", "rep", "tp"), None),
            P(("group", "rep", "tp"), None),
            P(),
            P(None, ("group", "rep"), None),
            P(None, ("group", "rep"), None),
            P(None, ("group", "rep"), None),
            P(("group", "rep"), "tp", None),
            P(("group", "rep"), "tp", None),
            P(("group", "rep"), None),
        ),
        out_specs=(
            P(("group", "rep", "tp"), None),
            P("tp"),
            P(None, ("group", "rep"), "tp"),
            P(None, ("group", "rep"), "tp"),
        ),
        check_vma=False,
    )
```
